128 devices in a mesh: grp: 4 (over z), wave: 32 (over x, y, core).
Axes of the slice: x: 4, y: 4, z: 4, core: 2. Of those that a mesh axis runs over, the one named last changes fastest.
Arguments:
- state: bfloat16 [275, 984320], P(None, ('grp', 'wave')), may hold values from -6 to 6
- held_orders: int32 [640], P(('grp', 'wave')), may hold values from -1 to 383, as said below
- pair_lows: int32 [384], P(('grp', 'wave')), may hold values from 0 to 383, each once
- inverses: bfloat16 [384, 2, 137, 137], P(('grp', 'wave')), may hold values from -2 to 3
- height_operator: bfloat16 [137, 137], replicated, may hold values from -0.5 to 0.5
- pressure_column: bfloat16 [137], replicated, may hold values from -5 to 5
- thermal_response_matrix: bfloat16 [137, 137], replicated, may hold values from -0.5 to 0.5
- mass_row: bfloat16 [137], replicated, may hold values from -0.5 to 0.5
Outputs:
- advanced: bfloat16 [275, 984320], P(None, ('grp', 'wave'))
The draws below stay inside these ranges and needn't reach their ends.
Inputs may be any that keep to these rules, and one draw needn't show every extreme that they name: `held_orders`: each of 0 to 383 appears exactly once, all other entries are -1; some device has all 5 of its slots filled.
All inputs are finite; a program needn't handle non-finite values.
Results may differ from the reference program's by a relative error of at most 0.0052.
Values may be sent and summed in bfloat16 or wider, within the bound.
A program may use at most 128 MiB of HBM per device.

```python
import jax
import jax.numpy as jnp
from jax import lax

LEVELS = 137
KMAX = 5
HALF = 384
TRUNC = 767
ORDER_SLOTS = 640
WIDTH_SLOT = 1538
COLS = 984320


def draw_held_orders(key, part):
    key_a, key_b, key_c = jax.random.split(jax.random.fold_in(key, 11), 3)
    slot_total = ORDER_SLOTS
    device_total = slot_total // KMAX
    scores = jax.random.permutation(key_a, slot_total).astype(jnp.int32)
    full_device = jax.random.randint(key_b, (), 0, device_total)
    owners = jnp.arange(slot_total, dtype=jnp.int32) // KMAX
    scores = scores - jnp.where(owners == full_device, slot_total, 0).astype(jnp.int32)
    ranking = jnp.argsort(jnp.argsort(scores))
    filled = ranking < HALF
    serial = jnp.cumsum(filled.astype(jnp.int32)) - 1
    orders = jax.random.permutation(key_c, HALF).astype(jnp.int32)
    picked = orders[jnp.clip(serial, 0, HALF - 1)]
    return jnp.where(filled, picked, -1).astype(jnp.int32)


def draw_inverses(key, part):
    key_a, key_b = jax.random.split(jax.random.fold_in(key, 23))
    diagonal = jax.random.uniform(key_a, (HALF, 2, LEVELS), jnp.float32, 0.6, 1.4)
    spread = jnp.clip(jax.random.normal(key_b, (HALF, 2, LEVELS, LEVELS), jnp.float32), -6.0, 6.0) * (0.6 / LEVELS ** 0.5)
    identity = jnp.eye(LEVELS, dtype=jnp.float32)
    return (spread + diagonal[..., None] * identity).astype(jnp.bfloat16)


def levels(rng, dims, pieces, low, top_value):
    level = 1.0
    for dim, parts in pieces:
        draws = jax.random.uniform(jax.random.fold_in(jax.random.fold_in(rng, 6), dim), (parts,), jnp.float32, low / len(pieces), top_value / len(pieces))
        level = level * jnp.repeat(jnp.exp(draws), dims[dim] // parts).reshape((-1,) + (1,) * (len(dims) - 1 - dim))
    return level


def noise(own_key, dims, deviation, most, pieces=(), held_as=jnp.bfloat16):
    loudness = levels(own_key, dims, pieces, -0.22, 0.18) if pieces else 1.0
    drawn = jax.random.normal(own_key, dims, jnp.float32) * deviation * loudness
    return jnp.minimum(jnp.maximum(drawn, -most), most).astype(held_as)


def setup_inputs(seed: int = 0) -> dict:
    splits = jax.random.split(jax.random.key(seed), 9)
    state = noise(splits[0], (2 * LEVELS + 1, COLS), 1.0, 6.0, ((1, 128),))
    held_orders = draw_held_orders(jax.random.fold_in(splits[8], 71), 0)
    pair_lows = jax.random.permutation(splits[2], HALF).astype(jnp.int32)
    inverses = draw_inverses(jax.random.fold_in(splits[8], 71), 0)
    height_operator = noise(splits[4], (LEVELS, LEVELS), LEVELS ** -0.5, 0.5)
    pressure_column = noise(splits[5], (LEVELS,), 1.0, 5.0)
    thermal_response_matrix = noise(splits[6], (LEVELS, LEVELS), LEVELS ** -0.5, 0.5)
    mass_row = noise(splits[7], (LEVELS,), LEVELS ** -0.5, 0.5)
    return {"state": state, "held_orders": held_orders, "pair_lows": pair_lows, "inverses": inverses, "height_operator": height_operator, "pressure_column": pressure_column, "thermal_response_matrix": thermal_response_matrix, "mass_row": mass_row}


def reference(state, held_orders, pair_lows, inverses, height_operator, pressure_column, thermal_response_matrix, mass_row):
    layer_heights_count = LEVELS
    truncation = TRUNC
    slot_width = WIDTH_SLOT
    slot_of = jnp.zeros((HALF,), jnp.int32).at[jnp.where(held_orders >= 0, held_orders, HALF)].set(
        jnp.arange(ORDER_SLOTS, dtype=jnp.int32), mode="drop")
    pair_of = jnp.zeros((HALF,), jnp.int32).at[pair_lows].set(jnp.arange(HALF, dtype=jnp.int32))
    coeff_index = jnp.arange(slot_width // 2, dtype=jnp.int32)
    denom = float(truncation * (truncation + 1))

    def pair_block(low_degree):
        high_degree = truncation - low_degree
        in_low = coeff_index <= low_degree
        degree = jnp.where(in_low, low_degree, high_degree)
        order_of = jnp.where(in_low, coeff_index, coeff_index - low_degree - 1)
        pair_m = jnp.minimum(order_of, truncation - order_of)
        position = jnp.where(order_of == pair_m, degree - order_of, degree + 1)
        first_col = slot_of[pair_m] * slot_width + 2 * position
        spectral_stacks = jnp.stack([first_col, first_col + 1], axis=1).reshape(-1).astype(jnp.int32)
        grouped_arrays = jnp.take(state, spectral_stacks, axis=1)
        divergence = grouped_arrays[:layer_heights_count]
        thermal_state_array = grouped_arrays[layer_heights_count:2 * layer_heights_count]
        pressure = grouped_arrays[2 * layer_heights_count]
        lap_scale = jnp.repeat((degree * (degree + 1)).astype(jnp.float32) / denom, 2)
        height_drive_term = jnp.dot(height_operator, thermal_state_array, preferred_element_type=jnp.float32)
        height_drive_term = height_drive_term + pressure_column.astype(jnp.float32)[:, None] * pressure.astype(jnp.float32)[None, :]
        right_side = (divergence.astype(jnp.float32) + lap_scale[None, :] * height_drive_term).astype(jnp.bfloat16)
        slot_pair = pair_of[low_degree]
        div_low = jnp.dot(inverses[slot_pair, 0], right_side, preferred_element_type=jnp.float32)
        div_high = jnp.dot(inverses[slot_pair, 1], right_side, preferred_element_type=jnp.float32)
        next_spreading_rate = jnp.where(jnp.repeat(in_low, 2)[None, :], div_low, div_high).astype(jnp.bfloat16)
        next_thermal_state = (thermal_state_array.astype(jnp.float32)
                    - jnp.dot(thermal_response_matrix, next_spreading_rate, preferred_element_type=jnp.float32)).astype(jnp.bfloat16)
        surface_mass_next = (pressure.astype(jnp.float32)
                     - jnp.dot(mass_row, next_spreading_rate, preferred_element_type=jnp.float32)).astype(jnp.bfloat16)
        return jnp.concatenate([next_spreading_rate, next_thermal_state, surface_mass_next[None, :]], axis=0), spectral_stacks

    blocks, spectral_stacks = lax.map(pair_block, jnp.arange(HALF, dtype=jnp.int32))
    rows = 2 * layer_heights_count + 1
    flat = jnp.transpose(blocks, (1, 0, 2)).reshape(rows, -1)
    result = jnp.zeros((rows, COLS), jnp.bfloat16)
    return result.at[:, spectral_stacks.reshape(-1)].set(flat)
```

```python
import functools

import jax
import jax.numpy as jnp
from jax import lax
from jax.experimental import pallas as pl
from jax.experimental.pallas import tpu as pltpu
from jax.sharding import Mesh
from jax.sharding import PartitionSpec as P

AXES = ("grp", "wave_0", "wave_1", "wave_2")
MESH = pl.DeviceIdType.MESH
BF16 = jnp.bfloat16
F32 = jnp.float32
LEV = 137
REM = LEV - 128
HALF = 384
TRUNC = 767
SLOTS = 5
WIDTH = 2 * (TRUNC + 2)
COLS = SLOTS * WIDTH
ROWS = 7696
PAIR_ROWS = 24
CHUNK = 8 * PAIR_ROWS
MSG = 224
UNIT = 320
LANES14 = 14
TILE = 1024
TILES = 8


def list_id(j, t, e):
    return j * 4 + t * 2 + e


def partner(core, p):
    even = p % 2
    return (1 - core) * (p + 1 - 2 * even) + core * (3 - p)


def solver_coords(pos, core, j, t, e):
    dest_core = (core + e) % 2
    pa = pos[j] if t == 0 else partner(dest_core, pos[j])
    return [pa if d == j else pos[d] for d in range(3)], dest_core


def source_coords(pos, core, j, rc, rb, ra):
    a, b, c = j, (j + 1) % 3, (j + 2) % 3
    out = [None, None, None]
    pa = pos[a]
    out[a] = pa + ra * (partner(1 - core, pa) - pa)
    out[b] = (pos[b] + 4 - rb) % 4
    out[c] = (pos[c] + 4 - rc) % 4
    return out


def slot_rows(low, order):
    first = jnp.where(order <= low, 2 * (low - order), 2 * (TRUNC + 1 - low))
    second = 2 * (TRUNC - low - order)
    return first, second


def pair_rows(low, orders, miss):
    rows = []
    extra = miss
    for s in range(SLOTS):
        first, second = slot_rows(low, orders[s])
        rows.append((2 * s, s * WIDTH + first))
        rows.append((2 * SLOTS + 2 * s, s * WIDTH + second))
        extra = jnp.where(orders[s] == low, s * WIDTH + 2 * (TRUNC + 1 - low), extra)
    rows.append((4 * SLOTS, extra))
    return rows


def exchange_kernel(
    units_hbm, meta_hbm, xm_hbm, xr_hbm, held,
    yr_out, meta_out,
    G, META, METAS, XM, XR, SND, RCV, YS, YR, TM, TR, MV, RA,
    in_sem, g_send, g_recv, m_send, m_recv, f_send, f_recv, b_send, b_recv, out_sem,
):
    pos = [lax.axis_index(AXES[d]) for d in range(3)]
    core = lax.axis_index(AXES[3])

    def device(coords, c):
        return {AXES[0]: coords[0], AXES[1]: coords[1], AXES[2]: coords[2], AXES[3]: c}

    def shifted(d, delta):
        return [(pos[k] + 4 + delta) % 4 if k == d else pos[k] for k in range(3)]

    own_meta = META.at[core, pos[2], pos[1], pos[0]]
    loads = [
        pltpu.make_async_copy(units_hbm, G.at[:, 0, 0, 0], in_sem.at[0]),
        pltpu.make_async_copy(meta_hbm, own_meta, in_sem.at[1]),
        pltpu.make_async_copy(xm_hbm, XM, in_sem.at[2]),
        pltpu.make_async_copy(xr_hbm, XR, in_sem.at[3]),
    ]
    for load in loads:
        load.start()

    barrier = pltpu.get_barrier_semaphore()
    peers = []
    for d in range(3):
        for delta in (1, -1):
            peers.append((shifted(d, delta), core))
            peers.append((shifted(d, delta), 1 - core))
        peers.append((shifted(d, 2), core))
    peers.append((pos, 1 - core))
    for coords, c in peers:
        pl.semaphore_signal(barrier, inc=1, device_id=device(coords, c), device_id_type=MESH)
    pl.semaphore_wait(barrier, len(peers))

    def unit_copy(j, dest):
        rc, rb, ra = dest
        a, b, c = j, (j + 1) % 3, (j + 2) % 3
        if dest == (0, 0, 1):
            src = (0, 0, 0)
            coords = [partner(1 - core, pos[k]) if k == a else pos[k] for k in range(3)]
        elif rc == 0:
            ring, step, k = b, rb, 1
        else:
            ring, step, k = c, rc, 0
        if dest != (0, 0, 1):
            forward = {1: (0, 1), 3: (0, -1), 2: (1, 1) if ra == 0 else (3, -1)}[step]
            src = list(dest)
            src[k] = forward[0]
            src = tuple(src)
            coords = shifted(ring, forward[1])
        return src, pltpu.make_async_remote_copy(
            src_ref=G.at[(j,) + src],
            dst_ref=G.at[(j,) + dest],
            send_sem=g_send.at[(j,) + dest],
            recv_sem=g_recv.at[(j,) + dest],
            device_id=device(coords, core),
            device_id_type=MESH,
        )

    here = {(j, 0, 0, 0) for j in range(3)}
    sent = []

    def need(j, unit):
        if (j,) + unit not in here:
            here.add((j,) + unit)
            unit_copy(j, unit)[1].wait_recv()

    def send(*dests):
        for dest in dests:
            for j in range(3):
                src, copy = unit_copy(j, dest)
                need(j, src)
                copy.start()
                sent.append(copy)

    def meta_copies(stage):
        out = []
        if stage < 3:
            d = stage
            index = (core, pos[2], pos[1], pos[0])[: 4 - d]
            for delta in (1, 2, 3):
                out.append((index, device(shifted(d, delta), core), 3 * d + delta - 1))
        else:
            out.append(((core,), device(pos, 1 - core), 9))
        return out

    def meta_copy(index, dev, sem):
        ref = META.at[index]
        return pltpu.make_async_remote_copy(
            src_ref=ref, dst_ref=ref, send_sem=m_send.at[sem], recv_sem=m_recv.at[sem],
            device_id=dev, device_id_type=MESH,
        )

    def meta_start(stage):
        for item in meta_copies(stage):
            copy = meta_copy(*item)
            copy.start()
            sent.append(copy)

    def meta_wait(stage):
        for item in meta_copies(stage):
            meta_copy(*item).wait_recv()

    loads[1].wait()
    meta_start(0)
    loads[0].wait()
    send((0, 0, 1), (0, 1, 0), (0, 3, 0), (1, 0, 0), (3, 0, 0))
    TM[...] = jnp.zeros_like(TM)
    TR[...] = jnp.zeros_like(TR)
    meta_wait(0)
    meta_start(1)
    meta_wait(1)
    meta_start(2)
    meta_wait(2)
    meta_start(3)
    send((0, 1, 1), (0, 3, 1), (1, 0, 1), (3, 0, 1))
    meta_wait(3)
    table = pltpu.make_async_copy(META, METAS, in_sem.at[4])
    table.start()
    meta_store = pltpu.make_async_copy(META, meta_out, in_sem.at[5])
    meta_store.start()
    table.wait()
    loads[2].wait()
    loads[3].wait()

    orders = [held[s] for s in range(SLOTS)]

    def low_of(coords, c, j):
        return METAS[c, coords[2], coords[1], coords[0], 0, j]

    def pack(j, t, e):
        dest, dest_core = solver_coords(pos, core, j, t, e)
        l = list_id(j, t, e)
        target = RCV if t + e == 0 else SND

        def body(rc, carry):
            for u in range(8):
                src = source_coords(dest, dest_core, j, rc, u // 2, u % 2)
                low = low_of(src, dest_core, j)
                for at, row in pair_rows(low, orders, 0):
                    put = PAIR_ROWS * u + at
                    TM[put : put + 2, :] = XM[pl.ds(row, 2), :]
                    TR[put : put + 2, :] = XR[pl.ds(row, 2), :]
            target[l, rc, 0:CHUNK, :] = TM[...].astype(BF16)
            tail = TR[0:PAIR_ROWS, :]
            for u in range(1, 8):
                tail += pltpu.roll(TR[PAIR_ROWS * u : PAIR_ROWS * (u + 1), :], 16 * u, 1)
            tail = jnp.concatenate([tail, jnp.zeros((MSG - CHUNK - PAIR_ROWS, 128), F32)], axis=0)
            target[l, rc, CHUNK:MSG, :] = tail.astype(BF16)
            return carry

        lax.fori_loop(0, 4, body, 0)
        if t + e:
            copy = forward_copy(j, t, e)
            copy.start()
            sent.append(copy)

    def forward_copy(j, t, e):
        dest, dest_core = solver_coords(pos, core, j, t, e)
        l = list_id(j, t, e)
        return pltpu.make_async_remote_copy(
            src_ref=SND.at[l], dst_ref=RCV.at[l], send_sem=f_send.at[l], recv_sem=f_recv.at[l],
            device_id=device(dest, dest_core), device_id_type=MESH,
        )

    def origin(j, t, e):
        pa = pos[j] if t == 0 else partner(core, pos[j])
        return [pa if d == j else pos[d] for d in range(3)], (core + e) % 2

    def return_copy(j, t, e, rc):
        l = list_id(j, t, e)
        coords, c = origin(j, t, e)
        return pltpu.make_async_remote_copy(
            src_ref=YS.at[l, rc], dst_ref=YR.at[l, rc], send_sem=b_send.at[l, rc], recv_sem=b_recv.at[l, rc],
            device_id=device(coords, c), device_id_type=MESH,
        )

    every = [(t, e) for t in (1, 0) for e in (0, 1)]
    row_id = lax.broadcasted_iota(jnp.int32, (PAIR_ROWS, 128), 0)

    def order_rows(j):
        for t, e in every:
            coords, c = origin(j, t, e)
            rows = jnp.full((PAIR_ROWS, 128), HALF + 1, jnp.int32)
            for s in range(SLOTS):
                order = METAS[c, coords[2], coords[1], coords[0], 0, 8 + s]
                rows = jnp.where(row_id // 2 == s, order, rows)
            MV[j, PAIR_ROWS * (2 * t + e) : PAIR_ROWS * (2 * t + e + 1), :] = rows

    lane = lax.broadcasted_iota(jnp.int32, (4 * PAIR_ROWS, 128), 1)

    def solve(j, rc):
        RA[...] = jnp.zeros_like(RA)

        def body(rb, carry):
            rows = pl.ds(pl.multiple_of(2 * PAIR_ROWS * rb, 16), 2 * PAIR_ROWS)
            mains = [RCV[list_id(j, k // 2, k % 2), rc, rows, :].astype(F32) for k in range(4)]
            tails = jnp.concatenate(
                [RCV[list_id(j, k // 2, k % 2), rc, CHUNK:MSG, :].astype(F32)[:PAIR_ROWS] for k in range(4)], axis=0
            )
            solved = []
            for ra in range(2):
                u = 2 * rb + ra
                low = low_of(source_coords(pos, core, j, rc, rb, ra), core, j)
                unit = G.at[j, rc, rb, ra]
                x = jnp.concatenate([m[PAIR_ROWS * ra : PAIR_ROWS * (ra + 1)] for m in mains], axis=0)
                is_low = MV[j] <= low
                main = jnp.concatenate([jnp.where(is_low, x, 0.0), jnp.where(is_low, 0.0, x)], axis=1).astype(BF16)
                tail_low = pltpu.roll(tails, (128 - 16 * u) % 128, 1)
                tail_high = pltpu.roll(tails, (144 - 16 * u) % 128, 1)
                tail = jnp.where(
                    lane < 16,
                    jnp.where(is_low, tail_low, 0.0),
                    jnp.where(lane < 32, jnp.where(is_low, 0.0, tail_high), 0.0),
                ).astype(BF16)
                strips = [unit[288:304, :].astype(F32), unit[304:320, :].astype(F32)]
                strip = jnp.concatenate(
                    [
                        pltpu.roll(strips[g // LANES14], (128 - REM * (g % LANES14)) % 128, 1)
                        for g in range(18)
                    ],
                    axis=0,
                ).astype(BF16)
                weights = jnp.concatenate([unit[0:256, :], strip[0:256]], axis=1)
                low_weights = jnp.concatenate([unit[256:288, :], strip[256:288]], axis=1)
                y = jnp.dot(main, weights, preferred_element_type=F32) + jnp.dot(
                    tail[:, 0:32], low_weights, preferred_element_type=F32
                )
                solved.append(y[:, 0:128])
                shifted_tail = pltpu.roll(y[:, 128:256], 16 * u, 1)
                keep = (lane >= 16 * u) & (lane < 16 * u + REM)
                RA[...] += jnp.where(keep, shifted_tail, 0.0)
            for k in range(4):
                l = list_id(j, k // 2, k % 2)
                part = slice(PAIR_ROWS * k, PAIR_ROWS * (k + 1))
                (YR if k == 0 else YS)[l, rc, rows, :] = jnp.concatenate(
                    [solved[0][part], solved[1][part]], axis=0
                ).astype(BF16)
            return carry

        lax.fori_loop(0, 4, body, 0)
        for k in range(4):
            l = list_id(j, k // 2, k % 2)
            part = jnp.concatenate(
                [RA[PAIR_ROWS * k : PAIR_ROWS * (k + 1), :], jnp.zeros((MSG - CHUNK - PAIR_ROWS, 128), F32)], axis=0
            )
            (YR if k == 0 else YS)[l, rc, CHUNK:MSG, :] = part.astype(BF16)
            if k:
                copy = return_copy(j, k // 2, k % 2, rc)
                copy.start()
                sent.append(copy)

    for j in range(3):
        pack(j, 1, 0)
        pack(j, 1, 1)
        if j == 0:
            send((0, 2, 0), (1, 1, 0), (3, 1, 0), (1, 3, 0), (3, 3, 0))
        elif j == 1:
            send((0, 2, 1), (1, 1, 1), (3, 1, 1), (1, 3, 1), (3, 3, 1))
        else:
            send((2, 0, 0), (2, 0, 1))
    for j in range(3):
        pack(j, 0, 1)
    send((1, 2, 0), (3, 2, 0), (1, 2, 1), (3, 2, 1))
    for j in range(3):
        pack(j, 0, 0)
        order_rows(j)
    send((2, 1, 0), (2, 1, 1), (2, 3, 0), (2, 3, 1))

    got = set()

    def solve_ready(j, rc):
        for t, e in every:
            if t + e and (j, t, e) not in got:
                got.add((j, t, e))
                forward_copy(j, t, e).wait_recv()
        for rb in range(4):
            for ra in range(2):
                need(j, (rc, rb, ra))
        solve(j, rc)

    for j in range(3):
        solve_ready(j, 0)
    send((2, 2, 0), (2, 2, 1))
    for rc in (1, 3, 2):
        for j in range(3):
            solve_ready(j, rc)
    for j in range(3):
        for rc in range(4):
            for t, e in every:
                if t + e:
                    return_copy(j, t, e, rc).wait_recv()
    done = pltpu.make_async_copy(YR, yr_out, out_sem)
    done.start()
    done.wait()
    meta_store.wait()
    for copy in sent:
        copy.wait_send()


def exchange(units, meta, xm, xr, held):
    any_space = pl.BlockSpec(memory_space=pl.ANY)
    messages = pltpu.VMEM((12, 4, MSG, 128), BF16)
    return pl.pallas_call(
        exchange_kernel,
        out_shape=(
            jax.ShapeDtypeStruct((12, 4, MSG, 128), BF16),
            jax.ShapeDtypeStruct((2, 4, 4, 4, 1, 128), jnp.int32),
        ),
        in_specs=[any_space] * 4 + [pl.BlockSpec(memory_space=pltpu.SMEM)],
        out_specs=(any_space, any_space),
        scratch_shapes=[
            pltpu.VMEM((3, 4, 4, 2, UNIT, 128), BF16),
            pltpu.VMEM((2, 4, 4, 4, 1, 128), jnp.int32),
            pltpu.SMEM((2, 4, 4, 4, 1, 128), jnp.int32),
            pltpu.VMEM((ROWS, 128), F32),
            pltpu.VMEM((ROWS, 128), F32),
            messages,
            messages,
            messages,
            messages,
            pltpu.VMEM((CHUNK, 128), F32),
            pltpu.VMEM((CHUNK, 128), F32),
            pltpu.VMEM((3, 4 * PAIR_ROWS, 128), jnp.int32),
            pltpu.VMEM((4 * PAIR_ROWS, 128), F32),
            pltpu.SemaphoreType.DMA((6,)),
            pltpu.SemaphoreType.DMA((3, 4, 4, 2)),
            pltpu.SemaphoreType.DMA((3, 4, 4, 2)),
            pltpu.SemaphoreType.DMA((10,)),
            pltpu.SemaphoreType.DMA((10,)),
            pltpu.SemaphoreType.DMA((12,)),
            pltpu.SemaphoreType.DMA((12,)),
            pltpu.SemaphoreType.DMA((12, 4)),
            pltpu.SemaphoreType.DMA((12, 4)),
            pltpu.SemaphoreType.DMA,
        ],
        compiler_params=pltpu.CompilerParams(
            collective_id=0, has_side_effects=True, vmem_limit_bytes=60 * 1024 * 1024
        ),
    )(units, meta, xm, xr, held)


def finish_kernel(yr, meta, held, place, state, live, am, ar, out, YM, YT, TM, TR):
    @pl.when(pl.program_id(0) == 0)
    def _():
        pos = [place[d] for d in range(3)]
        core = place[3]
        orders = [held[s] for s in range(SLOTS)]
        for j in range(3):
            for t in range(2):
                for e in range(2):
                    dest, dest_core = solver_coords(pos, core, j, t, e)
                    l = list_id(j, t, e)

                    def body(rc, carry):
                        TM[...] = yr[l, rc, 0:CHUNK, :].astype(F32)
                        tails = yr[l, rc, CHUNK:MSG, :].astype(F32)[0:PAIR_ROWS]
                        for u in range(8):
                            TR[PAIR_ROWS * u : PAIR_ROWS * (u + 1), :] = (
                                pltpu.roll(tails, 128 - 16 * u, 1) if u else tails
                            )
                        for u in range(8):
                            src = source_coords(dest, dest_core, j, rc, u // 2, u % 2)
                            low = meta[dest_core, src[2], src[1], src[0], 0, j]
                            for at, row in pair_rows(low, orders, TILE * TILES - 8):
                                put = PAIR_ROWS * u + at
                                YM[pl.ds(row, 2), :] = TM[put : put + 2, :]
                                YT[pl.ds(row, 2), :] = TR[put : put + 2, :]
                        return carry

                    lax.fori_loop(0, 4, body, 0)

    rows = pl.ds(pl.multiple_of(pl.program_id(0) * TILE, TILE), TILE)
    nt = (((1,), (1,)), ((), ()))
    lanes = lax.broadcasted_iota(jnp.int32, (TILE, 128), 1)
    tail = jnp.where(lanes < REM, YT[rows, :], 0.0).astype(BF16)
    total = lax.dot_general(am[...], YM[rows, :].astype(BF16), nt, preferred_element_type=F32)
    total += lax.dot_general(ar[...], tail, nt, preferred_element_type=F32)
    level = lax.broadcasted_iota(jnp.int32, total.shape, 0)
    total += jnp.where(level < LEV, 0.0, state[...].astype(F32))
    out[...] = jnp.where(live[...] > 0, total, 0.0).astype(BF16)


def finish(yr, meta, held, place, state, live, am, ar):
    smem = pl.BlockSpec(memory_space=pltpu.SMEM)
    rows = state.shape[0]
    block = pl.BlockSpec((rows, TILE), lambda i: (0, i))
    return pl.pallas_call(
        finish_kernel,
        grid=(TILES,),
        out_shape=jax.ShapeDtypeStruct(state.shape, BF16),
        in_specs=[
            pl.BlockSpec((12, 4, MSG, 128), lambda i: (0, 0, 0, 0)),
            smem,
            smem,
            smem,
            block,
            pl.BlockSpec((1, TILE), lambda i: (0, i)),
            pl.BlockSpec((rows, 128), lambda i: (0, 0)),
            pl.BlockSpec((rows, 128), lambda i: (0, 0)),
        ],
        out_specs=block,
        scratch_shapes=[
            pltpu.VMEM((TILE * TILES, 128), F32),
            pltpu.VMEM((TILE * TILES, 128), F32),
            pltpu.VMEM((CHUNK, 128), F32),
            pltpu.VMEM((CHUNK, 128), F32),
        ],
        compiler_params=pltpu.CompilerParams(vmem_limit_bytes=60 * 1024 * 1024),
    )(yr, meta, held, place, state, live, am, ar)


def unit_layout(inverses):
    turned = jnp.swapaxes(inverses, 2, 3)
    pad16 = ((0, 0), (0, 0), (0, 16 - REM), (0, 0))
    main = turned[:, :, :128, :128].reshape(3, 256, 128)
    bottom = jnp.pad(turned[:, :, 128:, :128], pad16).reshape(3, 32, 128)
    right = jnp.concatenate(
        [turned[:, :, :128, 128:].reshape(3, 256, REM), jnp.pad(turned[:, :, 128:, 128:], pad16).reshape(3, 32, REM)],
        axis=1,
    )
    groups = jnp.pad(right.reshape(3, 18, 16, REM), ((0, 0), (0, 2 * LANES14 - 18), (0, 0), (0, 0)))
    strips = groups.reshape(3, 2, LANES14, 16, REM).transpose(0, 1, 3, 2, 4).reshape(3, 32, LANES14 * REM)
    strips = jnp.pad(strips, ((0, 0), (0, 0), (0, 128 - LANES14 * REM)))
    return jnp.concatenate([main, bottom, strips], axis=1)


def shards(
    state,
    held_orders,
    pair_lows,
    inverses,
    height_operator,
    pressure_column,
    thermal_response_matrix,
    mass_row,
):
    denom = float(TRUNC * (TRUNC + 1))
    divergence = state[:LEV]
    thermal = state[LEV : 2 * LEV]
    pressure = state[2 * LEV]
    coeff = (jnp.arange(WIDTH, dtype=jnp.int32) // 2)[None, :]
    order_col = held_orders[:, None]
    degree = jnp.where(coeff <= TRUNC - order_col, order_col + coeff, coeff - 1)
    lap_scale = ((degree * (degree + 1)).astype(F32) / denom).reshape(-1)
    drive = lax.dot_general(thermal, height_operator, (((0,), (1,)), ((), ())), preferred_element_type=F32)
    drive = drive + pressure.astype(F32)[:, None] * pressure_column.astype(F32)[None, :]
    right_side = divergence.astype(F32).T + lap_scale[:, None] * drive
    xm = jnp.pad(right_side[:, :128], ((0, ROWS - COLS), (0, 0)))
    xr = jnp.pad(right_side[:, 128:], ((0, ROWS - COLS), (0, 128 - REM)))
    meta = jnp.zeros((1, 128), jnp.int32).at[0, 0:3].set(pair_lows).at[0, 8 : 8 + SLOTS].set(held_orders)
    yr, table = exchange(unit_layout(inverses), meta, xm, xr, held_orders)
    place = jnp.stack([lax.axis_index(name) for name in AXES]).astype(jnp.int32)
    live = jnp.repeat((held_orders >= 0).astype(F32), WIDTH)[None, :]
    operator = jnp.concatenate(
        [jnp.eye(LEV, dtype=BF16), -thermal_response_matrix, -mass_row[None, :]], axis=0
    )
    am = operator[:, :128]
    ar = jnp.pad(operator[:, 128:], ((0, 0), (0, 128 - REM)))
    return finish(yr, table, held_orders, place, state, live, am, ar)


def solution(mesh):
    torus = Mesh(mesh.devices.reshape(4, 4, 4, 2), AXES)
    columns = P(None, AXES)
    placed = (columns, P(AXES), P(AXES), P(AXES, None, None, None), P(), P(), P(), P())
    return jax.shard_map(shards, mesh=torus, in_specs=placed, out_specs=columns, check_vma=False)
```

```python
import functools

import jax
import jax.numpy as jnp
from jax import lax
from jax.experimental import pallas as pl
from jax.experimental.pallas import tpu as pltpu
from jax.sharding import Mesh
from jax.sharding import PartitionSpec as P

AXES = ("grp", "wave_0", "wave_1", "wave_2")
MESH = pl.DeviceIdType.MESH
BF16 = jnp.bfloat16
F32 = jnp.float32
LEV = 137
REM = LEV - 128
HALF = 384
TRUNC = 767
SLOTS = 5
WIDTH = 2 * (TRUNC + 2)
COLS = SLOTS * WIDTH
ROWS = 8192
MISS = ROWS - 8
PAIR_ROWS = 24
CHUNK = 8 * PAIR_ROWS
MSG = 224
UNIT = 320
STRIP = 2 * REM
PER_ROW = 7
BLOCK = 768
BLOCKS = 10
TAIL_COLS = COLS - BLOCK * BLOCKS
TILE = 1024
TILES = 8


def list_id(j, t, e):
    return j * 4 + t * 2 + e


def partner(core, p):
    even = p % 2
    return (1 - core) * (p + 1 - 2 * even) + core * (3 - p)


def solver_coords(pos, core, j, t, e):
    dest_core = (core + e) % 2
    pa = pos[j] if t == 0 else partner(dest_core, pos[j])
    return [pa if d == j else pos[d] for d in range(3)], dest_core


def source_coords(pos, core, j, rc, rb, ra):
    a, b, c = j, (j + 1) % 3, (j + 2) % 3
    out = [None, None, None]
    pa = pos[a]
    out[a] = pa + ra * (partner(1 - core, pa) - pa)
    out[b] = (pos[b] + 4 - rb) % 4
    out[c] = (pos[c] + 4 - rc) % 4
    return out


def copy_items(table, line, u, target, source):
    for t in range(2 * SLOTS + 1):
        put = PAIR_ROWS * u + 2 * t
        row = table[line, 16 * u + t]
        for to, of in zip(target, source):
            yield to, of, put, row


def exchange_kernel(
    inv_hbm, state_hbm, drive_hbm, lows, held,
    yr_out, table_out,
    RAW, STATE, DRIVE, G, META, METAS, TABLE, TABLES, XM, XR, SND, RCV, YS, YR, TM, TR, MV, RA,
    in_sem, g_send, g_recv, m_send, m_recv, f_send, f_recv, b_send, b_recv, out_sem,
):
    pos = [lax.axis_index(AXES[d]) for d in range(3)]
    core = lax.axis_index(AXES[3])

    def device(coords, c):
        return {AXES[0]: coords[0], AXES[1]: coords[1], AXES[2]: coords[2], AXES[3]: c}

    def shifted(d, delta):
        return [(pos[k] + 4 + delta) % 4 if k == d else pos[k] for k in range(3)]

    loads = [
        pltpu.make_async_copy(inv_hbm, RAW, in_sem.at[0]),
        pltpu.make_async_copy(drive_hbm, DRIVE, in_sem.at[1]),
        pltpu.make_async_copy(state_hbm, STATE, in_sem.at[2]),
    ]
    for load in loads:
        load.start()

    barrier = pltpu.get_barrier_semaphore()
    peers = []
    for d in range(3):
        for delta in (1, -1):
            peers.append((shifted(d, delta), core))
            peers.append((shifted(d, delta), 1 - core))
        peers.append((shifted(d, 2), core))
    peers.append((pos, 1 - core))
    for coords, c in peers:
        pl.semaphore_signal(barrier, inc=1, device_id=device(coords, c), device_id_type=MESH)

    lane1 = lax.broadcasted_iota(jnp.int32, (1, 128), 1)
    record = jnp.zeros((1, 128), jnp.int32)
    for k in range(3):
        record = jnp.where(lane1 == k, lows[k], record)
    for k in range(SLOTS):
        record = jnp.where(lane1 == 8 + k, held[k], record)
    META[core, pos[2], pos[1], pos[0]] = record
    loads[0].wait()
    for j in range(3):
        strips = [jnp.zeros((16, 128), F32)] * 2
        for h in range(2):
            G[j, 0, 0, 0, 128 * h : 128 * (h + 1), :] = RAW[j, h, 0:128, 0:128]
            G[j, 0, 0, 0, 256 + 16 * h : 272 + 16 * h, :] = RAW[j, h, 128:144, 0:128]
            for g in range(9):
                part = RAW[j, h, 16 * g : 16 * (g + 1), 128:256].astype(F32)
                shift = STRIP * (g % PER_ROW) + REM * h
                strips[g // PER_ROW] += pltpu.roll(part, shift, 1) if shift else part
        for k in range(2):
            G[j, 0, 0, 0, 288 + 16 * k : 304 + 16 * k, :] = strips[k].astype(BF16)
    pl.semaphore_wait(barrier, len(peers))

    def unit_copy(j, dest):
        rc, rb, ra = dest
        a, b, c = j, (j + 1) % 3, (j + 2) % 3
        if dest == (0, 0, 1):
            src = (0, 0, 0)
            coords = [partner(1 - core, pos[k]) if k == a else pos[k] for k in range(3)]
        elif rc == 0:
            ring, step, k = b, rb, 1
        else:
            ring, step, k = c, rc, 0
        if dest != (0, 0, 1):
            forward = {1: (0, 1), 3: (0, -1), 2: (1, 1) if ra == 0 else (3, -1)}[step]
            src = list(dest)
            src[k] = forward[0]
            src = tuple(src)
            coords = shifted(ring, forward[1])
        return src, pltpu.make_async_remote_copy(
            src_ref=G.at[(j,) + src],
            dst_ref=G.at[(j,) + dest],
            send_sem=g_send.at[(j,) + dest],
            recv_sem=g_recv.at[(j,) + dest],
            device_id=device(coords, core),
            device_id_type=MESH,
        )

    here = {(j, 0, 0, 0) for j in range(3)}
    sent = []

    def need(j, unit):
        if (j,) + unit not in here:
            here.add((j,) + unit)
            unit_copy(j, unit)[1].wait_recv()

    def send(*dests):
        for dest in dests:
            for j in range(3):
                src, copy = unit_copy(j, dest)
                need(j, src)
                copy.start()
                sent.append(copy)

    def meta_copies(stage):
        out = []
        if stage < 3:
            d = stage
            index = (core, pos[2], pos[1], pos[0])[: 4 - d]
            for delta in (1, 2, 3):
                out.append((index, device(shifted(d, delta), core), 3 * d + delta - 1))
        else:
            out.append(((core,), device(pos, 1 - core), 9))
        return out

    def meta_copy(index, dev, sem):
        ref = META.at[index]
        return pltpu.make_async_remote_copy(
            src_ref=ref, dst_ref=ref, send_sem=m_send.at[sem], recv_sem=m_recv.at[sem],
            device_id=dev, device_id_type=MESH,
        )

    def meta_start(stage):
        for item in meta_copies(stage):
            copy = meta_copy(*item)
            copy.start()
            sent.append(copy)

    def meta_wait(stage):
        for item in meta_copies(stage):
            meta_copy(*item).wait_recv()

    orders = [held[s] for s in range(SLOTS)]
    eye = (
        lax.broadcasted_iota(jnp.int32, (128, 128), 0) == lax.broadcasted_iota(jnp.int32, (128, 128), 1)
    ).astype(BF16)
    nt = (((1,), (1,)), ((), ()))

    def turn(all_rows, base, width):
        drive = jnp.dot(DRIVE[...], all_rows, preferred_element_type=F32)
        col = base + lax.broadcasted_iota(jnp.int32, (1, width), 1)
        order = jnp.full((1, width), orders[0], jnp.int32)
        start = jnp.zeros((1, width), jnp.int32)
        for s in range(1, SLOTS):
            order = jnp.where(col >= s * WIDTH, orders[s], order)
            start = jnp.where(col >= s * WIDTH, s * WIDTH, start)
        q = (col - start) // 2
        degree = jnp.where(q <= TRUNC - order, order + q, q - 1)
        scale = (degree * (degree + 1)).astype(F32) / float(TRUNC * (TRUNC + 1))
        level = lax.broadcasted_iota(jnp.int32, (144, width), 0)
        divergence = jnp.where(level < LEV, all_rows[0:144].astype(F32), 0.0)
        right = (divergence + scale * drive).astype(BF16)
        for k in range(width // 128):
            out = lax.dot_general(eye, right[:, 128 * k : 128 * (k + 1)], nt, preferred_element_type=F32)
            rows = pl.ds(pl.multiple_of(base + 128 * k, 128), 128)
            XM[rows, :] = out[:, 0:128]
            XR[rows, 0:16] = out[:, 128:144]

    def turn_blocks(first, last):
        def body(i, carry):
            base = pl.multiple_of(i * BLOCK, BLOCK)
            turn(STATE[:, pl.ds(base, BLOCK)], base, BLOCK)
            return carry

        lax.fori_loop(first, last, body, 0)

    meta_start(0)
    send((0, 0, 1), (0, 1, 0), (0, 3, 0), (1, 0, 0), (3, 0, 0))
    TM[...] = jnp.zeros_like(TM)
    TR[...] = jnp.zeros_like(TR)
    XM[MISS - 504 : ROWS, :] = jnp.zeros((512, 128), F32)
    XR[...] = jnp.zeros_like(XR)
    loads[1].wait()
    loads[2].wait()
    turn_blocks(0, 2)
    meta_wait(0)
    meta_start(1)
    send((0, 1, 1), (0, 3, 1), (1, 0, 1), (3, 0, 1))
    turn_blocks(2, 5)
    meta_wait(1)
    meta_start(2)
    send((0, 2, 0), (1, 1, 0), (3, 1, 0), (1, 3, 0), (3, 3, 0))
    turn_blocks(5, 8)
    meta_wait(2)
    meta_start(3)
    send((0, 2, 1), (1, 1, 1), (3, 1, 1), (1, 3, 1), (3, 3, 1))
    turn_blocks(8, 10)
    last = jnp.concatenate(
        [STATE[:, BLOCK * BLOCKS : COLS], jnp.zeros((2 * LEV + 1, 128 - TAIL_COLS), BF16)], axis=1
    )
    turn(last, BLOCK * BLOCKS, 128)
    meta_wait(3)
    send((2, 0, 0), (2, 0, 1))
    fetch = pltpu.make_async_copy(META, METAS, in_sem.at[3])
    fetch.start()
    fetch.wait()

    def low_of(coords, c, j):
        return METAS[c, coords[2], coords[1], coords[0], 0, j]

    every = [(t, e) for t in (1, 0) for e in (0, 1)]

    for j in range(3):
        for t, e in every:
            dest, dest_core = solver_coords(pos, core, j, t, e)
            for rc in range(4):
                line = jnp.zeros((1, 128), jnp.int32)
                for u in range(8):
                    src = source_coords(dest, dest_core, j, rc, u // 2, u % 2)
                    line = jnp.where(lane1 // 16 == u, low_of(src, dest_core, j), line)
                at = 4 * list_id(j, t, e) + rc
                TABLE[at : at + 1, :] = line
    low = TABLE[...]
    item = lax.broadcasted_iota(jnp.int32, (48, 128), 1) % 16
    order = jnp.zeros((48, 128), jnp.int32)
    extra = jnp.full((48, 128), MISS, jnp.int32)
    for s in range(SLOTS):
        order = jnp.where((item == s) | (item == SLOTS + s), orders[s], order)
        extra = jnp.where(low == orders[s], s * WIDTH + 2 * (TRUNC + 1 - low), extra)
    first = jnp.where(order <= low, 2 * (low - order), 2 * (TRUNC + 1 - low)) + item * WIDTH
    second = 2 * (TRUNC - low - order) + (item - SLOTS) * WIDTH
    TABLE[...] = jnp.where(item < SLOTS, first, jnp.where(item < 2 * SLOTS, second, extra))
    table = pltpu.make_async_copy(TABLE, TABLES, in_sem.at[4])
    table.start()
    table_store = pltpu.make_async_copy(TABLE, table_out, in_sem.at[5])
    table_store.start()
    table.wait()

    def pack(j, t, e):
        dest, dest_core = solver_coords(pos, core, j, t, e)
        l = list_id(j, t, e)
        target = RCV if t + e == 0 else SND

        def body(rc, carry):
            for u in range(8):
                for to, of, put, row in copy_items(TABLES, 4 * l + rc, u, (TM, TR), (XM, XR)):
                    to[put : put + 2, :] = of[pl.ds(row, 2), :]
            target[l, rc, 0:CHUNK, :] = TM[...].astype(BF16)
            tail = TR[0:PAIR_ROWS, :]
            for u in range(1, 8):
                tail += pltpu.roll(TR[PAIR_ROWS * u : PAIR_ROWS * (u + 1), :], 16 * u, 1)
            tail = jnp.concatenate([tail, jnp.zeros((MSG - CHUNK - PAIR_ROWS, 128), F32)], axis=0)
            target[l, rc, CHUNK:MSG, :] = tail.astype(BF16)
            return carry

        lax.fori_loop(0, 4, body, 0)
        if t + e:
            copy = forward_copy(j, t, e)
            copy.start()
            sent.append(copy)

    def forward_copy(j, t, e):
        dest, dest_core = solver_coords(pos, core, j, t, e)
        l = list_id(j, t, e)
        return pltpu.make_async_remote_copy(
            src_ref=SND.at[l], dst_ref=RCV.at[l], send_sem=f_send.at[l], recv_sem=f_recv.at[l],
            device_id=device(dest, dest_core), device_id_type=MESH,
        )

    def origin(j, t, e):
        pa = pos[j] if t == 0 else partner(core, pos[j])
        return [pa if d == j else pos[d] for d in range(3)], (core + e) % 2

    def return_copy(j, t, e, rc):
        l = list_id(j, t, e)
        coords, c = origin(j, t, e)
        return pltpu.make_async_remote_copy(
            src_ref=YS.at[l, rc], dst_ref=YR.at[l, rc], send_sem=b_send.at[l, rc], recv_sem=b_recv.at[l, rc],
            device_id=device(coords, c), device_id_type=MESH,
        )

    row_id = lax.broadcasted_iota(jnp.int32, (PAIR_ROWS, 128), 0)

    def order_rows(j):
        for t, e in every:
            coords, c = origin(j, t, e)
            rows = jnp.full((PAIR_ROWS, 128), HALF + 1, jnp.int32)
            for s in range(SLOTS):
                order = METAS[c, coords[2], coords[1], coords[0], 0, 8 + s]
                rows = jnp.where(row_id // 2 == s, order, rows)
            MV[j, PAIR_ROWS * (2 * t + e) : PAIR_ROWS * (2 * t + e + 1), :] = rows

    lane = lax.broadcasted_iota(jnp.int32, (4 * PAIR_ROWS, 128), 1)

    def solve(j, rc):
        RA[...] = jnp.zeros_like(RA)

        def body(rb, carry):
            rows = pl.ds(pl.multiple_of(2 * PAIR_ROWS * rb, 16), 2 * PAIR_ROWS)
            mains = [RCV[list_id(j, k // 2, k % 2), rc, rows, :].astype(F32) for k in range(4)]
            tails = jnp.concatenate(
                [RCV[list_id(j, k // 2, k % 2), rc, CHUNK:MSG, :].astype(F32)[:PAIR_ROWS] for k in range(4)], axis=0
            )
            solved = []
            for ra in range(2):
                u = 2 * rb + ra
                low = low_of(source_coords(pos, core, j, rc, rb, ra), core, j)
                unit = G.at[j, rc, rb, ra]
                x = jnp.concatenate([m[PAIR_ROWS * ra : PAIR_ROWS * (ra + 1)] for m in mains], axis=0)
                is_low = MV[j] <= low
                main = jnp.concatenate([jnp.where(is_low, x, 0.0), jnp.where(is_low, 0.0, x)], axis=1).astype(BF16)
                tail_low = pltpu.roll(tails, (128 - 16 * u) % 128, 1)
                tail_high = pltpu.roll(tails, (128 + REM - 16 * u) % 128, 1)
                tail = jnp.where(
                    lane < REM,
                    jnp.where(is_low, tail_low, 0.0),
                    jnp.where(lane < STRIP, jnp.where(is_low, 0.0, tail_high), 0.0),
                ).astype(BF16)
                strips = [unit[288:304, :].astype(F32), unit[304:320, :].astype(F32)]
                strip = jnp.concatenate(
                    [
                        pltpu.roll(strips[g // PER_ROW], (128 - STRIP * (g % PER_ROW)) % 128, 1)
                        for g in range(9)
                    ],
                    axis=0,
                ).astype(BF16)
                weights = jnp.concatenate(
                    [
                        jnp.concatenate([unit[0:128, :], unit[128:256, :]], axis=1),
                        jnp.concatenate([unit[256:272, :], unit[272:288, :]], axis=1),
                    ],
                    axis=0,
                )
                y = lax.dot_general(main, weights, nt, preferred_element_type=F32) + lax.dot_general(
                    tail, strip, nt, preferred_element_type=F32
                )
                solved.append(y[:, 0:128])
                wide = jnp.concatenate([y[:, 128:144], jnp.zeros((4 * PAIR_ROWS, 112), F32)], axis=1)
                shifted_tail = pltpu.roll(wide, 16 * u, 1)
                keep = (lane >= 16 * u) & (lane < 16 * u + REM)
                RA[...] += jnp.where(keep, shifted_tail, 0.0)
            for k in range(4):
                l = list_id(j, k // 2, k % 2)
                part = slice(PAIR_ROWS * k, PAIR_ROWS * (k + 1))
                (YR if k == 0 else YS)[l, rc, rows, :] = jnp.concatenate(
                    [solved[0][part], solved[1][part]], axis=0
                ).astype(BF16)
            return carry

        lax.fori_loop(0, 4, body, 0)
        for k in range(4):
            l = list_id(j, k // 2, k % 2)
            part = jnp.concatenate(
                [RA[PAIR_ROWS * k : PAIR_ROWS * (k + 1), :], jnp.zeros((MSG - CHUNK - PAIR_ROWS, 128), F32)], axis=0
            )
            (YR if k == 0 else YS)[l, rc, CHUNK:MSG, :] = part.astype(BF16)
            if k:
                copy = return_copy(j, k // 2, k % 2, rc)
                copy.start()
                sent.append(copy)

    for j in range(3):
        pack(j, 1, 0)
        pack(j, 1, 1)
    send((1, 2, 0), (3, 2, 0), (1, 2, 1), (3, 2, 1))
    for j in range(3):
        pack(j, 0, 1)
    send((2, 1, 0), (2, 1, 1), (2, 3, 0), (2, 3, 1))
    for j in range(3):
        pack(j, 0, 0)
        order_rows(j)

    got = set()

    def solve_ready(j, rc):
        for t, e in every:
            if t + e and (j, t, e) not in got:
                got.add((j, t, e))
                forward_copy(j, t, e).wait_recv()
        for rb in range(4):
            for ra in range(2):
                need(j, (rc, rb, ra))
        solve(j, rc)

    for j in range(3):
        solve_ready(j, 0)
    send((2, 2, 0), (2, 2, 1))
    for rc in (1, 3, 2):
        for j in range(3):
            solve_ready(j, rc)
    stores = []
    for j in range(3):
        for t, e in every:
            for rc in range(4):
                if t + e:
                    return_copy(j, t, e, rc).wait_recv()
            l = list_id(j, t, e)
            stores.append(pltpu.make_async_copy(YR.at[l], yr_out.at[l], out_sem.at[l]))
            stores[-1].start()
    for store in stores:
        store.wait()
    table_store.wait()
    for copy in sent:
        copy.wait_send()


def exchange(inverses, state, drive, lows, held):
    any_space = pl.BlockSpec(memory_space=pl.ANY)
    smem = pl.BlockSpec(memory_space=pltpu.SMEM)
    messages = pltpu.VMEM((12, 4, MSG, 128), BF16)
    return pl.pallas_call(
        exchange_kernel,
        out_shape=(
            jax.ShapeDtypeStruct((12, 4, MSG, 128), BF16),
            jax.ShapeDtypeStruct((48, 128), jnp.int32),
        ),
        in_specs=[any_space] * 3 + [smem, smem],
        out_specs=(any_space, any_space),
        scratch_shapes=[
            pltpu.VMEM(inverses.shape, BF16),
            pltpu.VMEM(state.shape, BF16),
            pltpu.VMEM(drive.shape, BF16),
            pltpu.VMEM((3, 4, 4, 2, UNIT, 128), BF16),
            pltpu.VMEM((2, 4, 4, 4, 1, 128), jnp.int32),
            pltpu.SMEM((2, 4, 4, 4, 1, 128), jnp.int32),
            pltpu.VMEM((48, 128), jnp.int32),
            pltpu.SMEM((48, 128), jnp.int32),
            pltpu.VMEM((ROWS, 128), F32),
            pltpu.VMEM((ROWS, 128), F32),
            messages,
            messages,
            messages,
            messages,
            pltpu.VMEM((CHUNK, 128), F32),
            pltpu.VMEM((CHUNK, 128), F32),
            pltpu.VMEM((3, 4 * PAIR_ROWS, 128), jnp.int32),
            pltpu.VMEM((4 * PAIR_ROWS, 128), F32),
            pltpu.SemaphoreType.DMA((6,)),
            pltpu.SemaphoreType.DMA((3, 4, 4, 2)),
            pltpu.SemaphoreType.DMA((3, 4, 4, 2)),
            pltpu.SemaphoreType.DMA((10,)),
            pltpu.SemaphoreType.DMA((10,)),
            pltpu.SemaphoreType.DMA((12,)),
            pltpu.SemaphoreType.DMA((12,)),
            pltpu.SemaphoreType.DMA((12, 4)),
            pltpu.SemaphoreType.DMA((12, 4)),
            pltpu.SemaphoreType.DMA((12,)),
        ],
        compiler_params=pltpu.CompilerParams(
            collective_id=0, has_side_effects=True, vmem_limit_bytes=60 * 1024 * 1024
        ),
    )(inverses, state, drive, lows, held)


def finish_kernel(yr, table, held, state, operator, out, YM, YT, TM, TR):
    @pl.when(pl.program_id(0) == 0)
    def _():
        def body(line, carry):
            l, rc = line // 4, line % 4
            TM[...] = yr[l, rc, 0:CHUNK, :].astype(F32)
            tails = yr[l, rc, CHUNK:MSG, :].astype(F32)[0:PAIR_ROWS]
            for u in range(8):
                TR[PAIR_ROWS * u : PAIR_ROWS * (u + 1), :] = pltpu.roll(tails, 128 - 16 * u, 1) if u else tails
            for u in range(8):
                for to, of, put, row in copy_items(table, line, u, (YM, YT), (TM, TR)):
                    to[pl.ds(row, 2), :] = of[put : put + 2, :]
            return carry

        lax.fori_loop(0, 48, body, 0)

    rows = pl.ds(pl.multiple_of(pl.program_id(0) * TILE, TILE), TILE)
    nt = (((1,), (1,)), ((), ()))
    lanes = lax.broadcasted_iota(jnp.int32, (TILE, 128), 1)
    tail = jnp.where(lanes < REM, YT[rows, :], 0.0).astype(BF16)
    total = lax.dot_general(operator[:, 0:128], YM[rows, :].astype(BF16), nt, preferred_element_type=F32)
    total += lax.dot_general(operator[:, 128:256], tail, nt, preferred_element_type=F32)
    level = lax.broadcasted_iota(jnp.int32, total.shape, 0)
    total += jnp.where(level < LEV, 0.0, state[...].astype(F32))
    col = pl.program_id(0) * TILE + lax.broadcasted_iota(jnp.int32, (1, TILE), 1)
    order = jnp.full((1, TILE), held[0], jnp.int32)
    for s in range(1, SLOTS):
        order = jnp.where(col >= s * WIDTH, held[s], order)
    out[...] = jnp.where(order >= 0, total, 0.0).astype(BF16)


def finish(yr, table, held, state, operator):
    smem = pl.BlockSpec(memory_space=pltpu.SMEM)
    rows = state.shape[0]
    block = pl.BlockSpec((rows, TILE), lambda i: (0, i))
    return pl.pallas_call(
        finish_kernel,
        grid=(TILES,),
        out_shape=jax.ShapeDtypeStruct(state.shape, BF16),
        in_specs=[
            pl.BlockSpec((12, 4, MSG, 128), lambda i: (0, 0, 0, 0)),
            smem,
            smem,
            block,
            pl.BlockSpec((rows, 256), lambda i: (0, 0)),
        ],
        out_specs=block,
        scratch_shapes=[
            pltpu.VMEM((TILE * TILES, 128), F32),
            pltpu.VMEM((TILE * TILES, 128), F32),
            pltpu.VMEM((CHUNK, 128), F32),
            pltpu.VMEM((CHUNK, 128), F32),
        ],
        compiler_params=pltpu.CompilerParams(vmem_limit_bytes=60 * 1024 * 1024),
    )(yr, table, held, state, operator)


def shards(
    state,
    held_orders,
    pair_lows,
    inverses,
    height_operator,
    pressure_column,
    thermal_response_matrix,
    mass_row,
):
    padded = jnp.pad(inverses, ((0, 0), (0, 0), (0, 144 - LEV), (0, 256 - LEV)))
    drive = jnp.concatenate([jnp.zeros((LEV, LEV), BF16), height_operator, pressure_column[:, None]], axis=1)
    drive = jnp.pad(drive, ((0, 144 - LEV), (0, 0)))
    yr, table = exchange(padded, state, drive, pair_lows, held_orders)
    operator = jnp.concatenate([jnp.eye(LEV, dtype=BF16), -thermal_response_matrix, -mass_row[None, :]], axis=0)
    operator = jnp.pad(operator, ((0, 0), (0, 256 - LEV)))
    return finish(yr, table, held_orders, state, operator)


def solution(mesh):
    torus = Mesh(mesh.devices.reshape(4, 4, 4, 2), AXES)
    columns = P(None, AXES)
    placed = (columns, P(AXES), P(AXES), P(AXES, None, None, None), P(), P(), P(), P())
    return jax.shard_map(shards, mesh=torus, in_specs=placed, out_specs=columns, check_vma=False)
```

```python
import functools

import jax
import jax.numpy as jnp
from jax import lax
from jax.experimental import pallas as pl
from jax.experimental.pallas import tpu as pltpu
from jax.sharding import Mesh
from jax.sharding import PartitionSpec as P

AXES = ("grp", "wave_0", "wave_1", "wave_2")
MESH = pl.DeviceIdType.MESH
BF16 = jnp.bfloat16
F32 = jnp.float32
LEV = 137
REM = LEV - 128
HALF = 384
TRUNC = 767
SLOTS = 5
WIDTH = 2 * (TRUNC + 2)
COLS = SLOTS * WIDTH
ROWS = 8192
MISS = ROWS - 8
PAIR_ROWS = 24
CHUNK = 8 * PAIR_ROWS
MSG = 224
UNIT = 320
STRIP = 2 * REM
PER_ROW = 7
BLOCK = 768
BLOCKS = 10
TAIL_COLS = COLS - BLOCK * BLOCKS
TILE = 1024
TILES = 8


def list_id(j, t, e):
    return j * 4 + t * 2 + e


def partner(core, p):
    even = p % 2
    return (1 - core) * (p + 1 - 2 * even) + core * (3 - p)


def solver_coords(pos, core, j, t, e):
    dest_core = (core + e) % 2
    pa = pos[j] if t == 0 else partner(dest_core, pos[j])
    return [pa if d == j else pos[d] for d in range(3)], dest_core


def source_coords(pos, core, j, rc, rb, ra):
    a, b, c = j, (j + 1) % 3, (j + 2) % 3
    out = [None, None, None]
    pa = pos[a]
    out[a] = pa + ra * (partner(1 - core, pa) - pa)
    out[b] = (pos[b] + 4 - rb) % 4
    out[c] = (pos[c] + 4 - rc) % 4
    return out


def copy_items(table, line, u, target, source):
    for t in range(2 * SLOTS + 1):
        put = PAIR_ROWS * u + 2 * t
        row = table[line, 16 * u + t]
        for to, of in zip(target, source):
            yield to, of, put, row


def exchange_kernel(
    inv_hbm, state_hbm, height, pressure, lows, held,
    yr_out, table_out,
    RAW, STATE, DRIVE, G, META, METAS, TABLE, TABLES, XM, XR, SND, RCV, YS, YR, TM, TR, MV,
    in_sem, g_send, g_recv, m_send, m_recv, f_send, f_recv, b_send, b_recv, out_sem,
):
    pos = [lax.axis_index(AXES[d]) for d in range(3)]
    core = lax.axis_index(AXES[3])

    def device(coords, c):
        return {AXES[0]: coords[0], AXES[1]: coords[1], AXES[2]: coords[2], AXES[3]: c}

    def shifted(d, delta):
        return [(pos[k] + 4 + delta) % 4 if k == d else pos[k] for k in range(3)]

    loads = [
        pltpu.make_async_copy(inv_hbm, RAW, in_sem.at[0]),
        pltpu.make_async_copy(state_hbm, STATE, in_sem.at[1]),
    ]
    for load in loads:
        load.start()

    barrier = pltpu.get_barrier_semaphore()
    other = 1 - core
    peers = [(pos, other)]
    for d in range(3):
        for delta in (1, -1):
            peers.append((shifted(d, delta), core))
            peers.append((shifted(d, delta), other))
        peers.append((shifted(d, 2), core))
    peers.append((shifted(0, 2), other))

    for coords, c in peers:
        pl.semaphore_signal(barrier, inc=1, device_id=device(coords, c), device_id_type=MESH)

    lane1 = lax.broadcasted_iota(jnp.int32, (1, 128), 1)
    record = jnp.zeros((1, 128), jnp.int32)
    for k in range(3):
        record = jnp.where(lane1 == k, lows[k], record)
    for k in range(SLOTS):
        record = jnp.where(lane1 == 8 + k, held[k], record)
    META[pos[2], pos[1], core, pos[0]] = record

    def chosen(rows, cols, test):
        r = lax.broadcasted_iota(jnp.int32, (rows, cols), 0)
        c = lax.broadcasted_iota(jnp.int32, (rows, cols), 1)
        return test(r, c).astype(BF16)

    below = chosen(16, LEV, lambda r, c: c == r + 128)
    beside = chosen(LEV, 128, lambda r, c: r == c + 128)
    loads[0].wait()
    for j in range(3):
        strips = [jnp.zeros((16, 128), F32)] * 2
        for h in range(2):
            raw = RAW[j, :, h, :]
            bottom = jnp.dot(below, raw, preferred_element_type=F32).astype(BF16)
            right = jnp.dot(raw, beside, preferred_element_type=F32)
            corner = jnp.dot(bottom, beside, preferred_element_type=F32)
            G[j, 0, 0, 0, 128 * h : 128 * (h + 1), :] = raw[0:128, 0:128]
            G[j, 0, 0, 0, 256 + 16 * h : 272 + 16 * h, :] = bottom[:, 0:128]
            for g in range(9):
                part = right[16 * g : 16 * (g + 1)] if g < 8 else corner
                shift = STRIP * (g % PER_ROW) + REM * h
                strips[g // PER_ROW] += pltpu.roll(part, shift, 1) if shift else part
        for k in range(2):
            G[j, 0, 0, 0, 288 + 16 * k : 304 + 16 * k, :] = strips[k].astype(BF16)
    pl.semaphore_wait(barrier, len(peers))

    def unit_copy(j, dest):
        rc, rb, ra = dest
        a, b, c = j, (j + 1) % 3, (j + 2) % 3
        if dest == (0, 0, 1):
            src = (0, 0, 0)
            coords = [partner(1 - core, pos[k]) if k == a else pos[k] for k in range(3)]
        elif rc == 0:
            ring, step, k = b, rb, 1
        else:
            ring, step, k = c, rc, 0
        if dest != (0, 0, 1):
            forward = {1: (0, 1), 3: (0, -1), 2: (1, 1) if ra == 0 else (3, -1)}[step]
            src = list(dest)
            src[k] = forward[0]
            src = tuple(src)
            coords = shifted(ring, forward[1])
        return src, pltpu.make_async_remote_copy(
            src_ref=G.at[(j,) + src],
            dst_ref=G.at[(j,) + dest],
            send_sem=g_send.at[(j,) + dest],
            recv_sem=g_recv.at[(j,) + dest],
            device_id=device(coords, core),
            device_id_type=MESH,
        )

    here = {(j, 0, 0, 0) for j in range(3)}
    sent = []

    def need(j, unit):
        if (j,) + unit not in here:
            here.add((j,) + unit)
            unit_copy(j, unit)[1].wait_recv()

    def send(*dests):
        for dest in dests:
            for j in range(3):
                src, copy = unit_copy(j, dest)
                need(j, src)
                copy.start()
                sent.append(copy)

    def meta_copies(stage):
        if stage == 0:
            index = (pos[2], pos[1], core, pos[0])
            out = [(index, device(shifted(0, delta), core), delta - 1) for delta in (1, 2, 3)]
            return out + [(index, device(shifted(0, delta), other), 3 + delta) for delta in range(4)]
        index = (pos[2], pos[1])[: 3 - stage]
        return [(index, device(shifted(stage, delta), core), 3 + 3 * stage + delta) for delta in (1, 2, 3)]

    def meta_copy(index, dev, sem):
        ref = META.at[index]
        return pltpu.make_async_remote_copy(
            src_ref=ref, dst_ref=ref, send_sem=m_send.at[sem], recv_sem=m_recv.at[sem],
            device_id=dev, device_id_type=MESH,
        )

    def meta_start(stage):
        for item in meta_copies(stage):
            copy = meta_copy(*item)
            copy.start()
            sent.append(copy)

    def meta_wait(stage):
        for item in meta_copies(stage):
            meta_copy(*item).wait_recv()

    orders = [held[s] for s in range(SLOTS)]
    eye = (
        lax.broadcasted_iota(jnp.int32, (128, 128), 0) == lax.broadcasted_iota(jnp.int32, (128, 128), 1)
    ).astype(BF16)
    nt = (((1,), (1,)), ((), ()))

    def turn(all_rows, base, width):
        drive = jnp.dot(DRIVE[0:144, :], all_rows, preferred_element_type=F32)
        col = base + lax.broadcasted_iota(jnp.int32, (1, width), 1)
        order = jnp.full((1, width), orders[0], jnp.int32)
        start = jnp.zeros((1, width), jnp.int32)
        for s in range(1, SLOTS):
            order = jnp.where(col >= s * WIDTH, orders[s], order)
            start = jnp.where(col >= s * WIDTH, s * WIDTH, start)
        q = (col - start) // 2
        degree = jnp.where(q <= TRUNC - order, order + q, q - 1)
        scale = (degree * (degree + 1)).astype(F32) / float(TRUNC * (TRUNC + 1))
        level = lax.broadcasted_iota(jnp.int32, (144, width), 0)
        divergence = jnp.where(level < LEV, all_rows[0:144].astype(F32), 0.0)
        right = (divergence + scale * drive).astype(BF16)
        for k in range(width // 128):
            out = lax.dot_general(eye, right[:, 128 * k : 128 * (k + 1)], nt, preferred_element_type=F32)
            rows = pl.ds(pl.multiple_of(base + 128 * k, 128), 128)
            XM[rows, :] = out[:, 0:128]
            XR[rows, 0:16] = out[:, 128:144]

    def turn_blocks(first, last):
        def body(i, carry):
            base = pl.multiple_of(i * BLOCK, BLOCK)
            turn(STATE[:, pl.ds(base, BLOCK)], base, BLOCK)
            return carry

        lax.fori_loop(first, last, body, 0)

    meta_start(0)
    send((0, 0, 1), (0, 1, 0), (0, 3, 0), (1, 0, 0), (3, 0, 0))
    TM[...] = jnp.zeros_like(TM)
    TR[...] = jnp.zeros_like(TR)
    XM[MISS - 504 : ROWS, :] = jnp.zeros((512, 128), F32)
    XR[...] = jnp.zeros_like(XR)
    rows = 2 * LEV + 1
    diagonal = chosen(LEV, LEV, lambda r, c: r == c) * jnp.broadcast_to(pressure[...][None, :], (LEV, LEV))
    thermal_rows = chosen(LEV, rows, lambda r, c: c == r + LEV)
    pressure_row = chosen(LEV, rows, lambda r, c: c == 2 * LEV)
    DRIVE[...] = jnp.zeros_like(DRIVE)
    DRIVE[0:LEV, :] = (
        jnp.dot(height[...], thermal_rows, preferred_element_type=F32)
        + jnp.dot(diagonal, pressure_row, preferred_element_type=F32)
    ).astype(BF16)
    loads[1].wait()
    turn_blocks(0, 7)
    meta_wait(0)
    meta_start(1)
    send((0, 1, 1), (0, 3, 1), (1, 0, 1), (3, 0, 1))
    turn_blocks(7, 10)
    last = jnp.concatenate([STATE[:, BLOCK * BLOCKS : COLS], jnp.zeros((rows, 128 - TAIL_COLS), BF16)], axis=1)
    turn(last, BLOCK * BLOCKS, 128)
    meta_wait(1)
    meta_start(2)
    send((0, 2, 0), (1, 1, 0), (3, 1, 0), (1, 3, 0), (3, 3, 0))
    send((0, 2, 1), (1, 1, 1), (3, 1, 1), (1, 3, 1), (3, 3, 1))
    meta_wait(2)
    fetch = pltpu.make_async_copy(META, METAS, in_sem.at[2])
    fetch.start()

    def low_of(coords, c, j):
        return METAS[coords[2], coords[1], c, coords[0], 0, j]

    every = [(t, e) for t in (1, 0) for e in (0, 1)]

    for j in range(3):
        for t, e in every:
            dest, dest_core = solver_coords(pos, core, j, t, e)
            for rc in range(4):
                line = jnp.zeros((1, 128), jnp.int32)
                for u in range(8):
                    src = source_coords(dest, dest_core, j, rc, u // 2, u % 2)
                    entry = META[src[2], src[1], dest_core, src[0]]
                    line = jnp.where(lane1 // 16 == u, jnp.broadcast_to(entry[:, j : j + 1], (1, 128)), line)
                at = 4 * list_id(j, t, e) + rc
                TABLE[at : at + 1, :] = line
    low = TABLE[...]
    item = lax.broadcasted_iota(jnp.int32, (48, 128), 1) % 16
    order = jnp.zeros((48, 128), jnp.int32)
    extra = jnp.full((48, 128), MISS, jnp.int32)
    for s in range(SLOTS):
        order = jnp.where((item == s) | (item == SLOTS + s), orders[s], order)
        extra = jnp.where(low == orders[s], s * WIDTH + 2 * (TRUNC + 1 - low), extra)
    first = jnp.where(order <= low, 2 * (low - order), 2 * (TRUNC + 1 - low)) + item * WIDTH
    second = 2 * (TRUNC - low - order) + (item - SLOTS) * WIDTH
    TABLE[...] = jnp.where(item < SLOTS, first, jnp.where(item < 2 * SLOTS, second, extra))
    table = pltpu.make_async_copy(TABLE, TABLES, in_sem.at[3])
    table.start()
    table_store = pltpu.make_async_copy(TABLE, table_out, in_sem.at[4])
    table_store.start()
    send((2, 0, 0), (2, 0, 1))
    table.wait()

    def pack(j, t, e):
        dest, dest_core = solver_coords(pos, core, j, t, e)
        l = list_id(j, t, e)
        target = RCV if t + e == 0 else SND

        for rc in range(4):
            for u in range(8):
                for to, of, put, row in copy_items(TABLES, 4 * l + rc, u, (TM.at[rc], TR.at[rc]), (XM, XR)):
                    to[put : put + 2, :] = of[pl.ds(row, 2), :]
            target[l, rc, 0:CHUNK, :] = TM[rc].astype(BF16)
            tail = TR[rc, 0:PAIR_ROWS, :]
            for u in range(1, 8):
                tail += pltpu.roll(TR[rc, PAIR_ROWS * u : PAIR_ROWS * (u + 1), :], 16 * u, 1)
            tail = jnp.concatenate([tail, jnp.zeros((MSG - CHUNK - PAIR_ROWS, 128), F32)], axis=0)
            target[l, rc, CHUNK:MSG, :] = tail.astype(BF16)

        if t + e:
            copy = forward_copy(j, t, e)
            copy.start()
            sent.append(copy)

    def forward_copy(j, t, e):
        dest, dest_core = solver_coords(pos, core, j, t, e)
        l = list_id(j, t, e)
        return pltpu.make_async_remote_copy(
            src_ref=SND.at[l], dst_ref=RCV.at[l], send_sem=f_send.at[l], recv_sem=f_recv.at[l],
            device_id=device(dest, dest_core), device_id_type=MESH,
        )

    def origin(j, t, e):
        pa = pos[j] if t == 0 else partner(core, pos[j])
        return [pa if d == j else pos[d] for d in range(3)], (core + e) % 2

    def return_copy(j, t, e, rc):
        l = list_id(j, t, e)
        coords, c = origin(j, t, e)
        return pltpu.make_async_remote_copy(
            src_ref=YS.at[l, rc], dst_ref=YR.at[l, rc], send_sem=b_send.at[l, rc], recv_sem=b_recv.at[l, rc],
            device_id=device(coords, c), device_id_type=MESH,
        )

    row_id = lax.broadcasted_iota(jnp.int32, (PAIR_ROWS, 128), 0)

    def order_rows(j):
        for t, e in every:
            coords, c = origin(j, t, e)
            rows = jnp.full((PAIR_ROWS, 128), HALF + 1, jnp.int32)
            for s in range(SLOTS):
                order = METAS[coords[2], coords[1], c, coords[0], 0, 8 + s]
                rows = jnp.where(row_id // 2 == s, order, rows)
            MV[j, PAIR_ROWS * (2 * t + e) : PAIR_ROWS * (2 * t + e + 1), :] = rows

    lane = lax.broadcasted_iota(jnp.int32, (4 * PAIR_ROWS, 128), 1)

    def solve(j, rc):
        tails = jnp.concatenate(
            [RCV[list_id(j, k // 2, k % 2), rc, CHUNK:MSG, :].astype(F32)[:PAIR_ROWS] for k in range(4)], axis=0
        )
        spread = jnp.zeros((4 * PAIR_ROWS, 128), F32)
        for rb in range(4):
            rows = slice(2 * PAIR_ROWS * rb, 2 * PAIR_ROWS * (rb + 1))
            mains = [RCV[list_id(j, k // 2, k % 2), rc, rows, :].astype(F32) for k in range(4)]
            solved = []
            for ra in range(2):
                u = 2 * rb + ra
                low = low_of(source_coords(pos, core, j, rc, rb, ra), core, j)
                unit = G.at[j, rc, rb, ra]
                x = jnp.concatenate([m[PAIR_ROWS * ra : PAIR_ROWS * (ra + 1)] for m in mains], axis=0)
                is_low = MV[j] <= low
                main = jnp.concatenate([jnp.where(is_low, x, 0.0), jnp.where(is_low, 0.0, x)], axis=1).astype(BF16)
                tail_low = pltpu.roll(tails, 128 - 16 * u, 1) if u else tails
                tail_high = pltpu.roll(tails, (128 + REM - 16 * u) % 128, 1)
                tail = jnp.where(
                    lane < REM,
                    jnp.where(is_low, tail_low, 0.0),
                    jnp.where(lane < STRIP, jnp.where(is_low, 0.0, tail_high), 0.0),
                ).astype(BF16)
                strips = [unit[288:304, :].astype(F32), unit[304:320, :].astype(F32)]
                strip = jnp.concatenate(
                    [
                        pltpu.roll(strips[g // PER_ROW], 128 - STRIP * (g % PER_ROW), 1)
                        if g % PER_ROW
                        else strips[g // PER_ROW]
                        for g in range(9)
                    ],
                    axis=0,
                ).astype(BF16)
                weights = jnp.concatenate(
                    [
                        jnp.concatenate([unit[0:128, :], unit[128:256, :]], axis=1),
                        jnp.concatenate([unit[256:272, :], unit[272:288, :]], axis=1),
                    ],
                    axis=0,
                )
                y = lax.dot_general(main, weights, nt, preferred_element_type=F32) + lax.dot_general(
                    tail, strip, nt, preferred_element_type=F32
                )
                solved.append(y[:, 0:128])
                wide = jnp.concatenate([y[:, 128:144], jnp.zeros((4 * PAIR_ROWS, 112), F32)], axis=1)
                shifted_tail = pltpu.roll(wide, 16 * u, 1) if u else wide
                keep = (lane >= 16 * u) & (lane < 16 * u + REM)
                spread += jnp.where(keep, shifted_tail, 0.0)
            for k in range(4):
                l = list_id(j, k // 2, k % 2)
                part = slice(PAIR_ROWS * k, PAIR_ROWS * (k + 1))
                (YR if k == 0 else YS)[l, rc, rows, :] = jnp.concatenate(
                    [solved[0][part], solved[1][part]], axis=0
                ).astype(BF16)
        for k in range(4):
            l = list_id(j, k // 2, k % 2)
            part = jnp.concatenate(
                [spread[PAIR_ROWS * k : PAIR_ROWS * (k + 1), :], jnp.zeros((MSG - CHUNK - PAIR_ROWS, 128), F32)], axis=0
            )
            (YR if k == 0 else YS)[l, rc, CHUNK:MSG, :] = part.astype(BF16)
            if k:
                copy = return_copy(j, k // 2, k % 2, rc)
                copy.start()
                sent.append(copy)

    pack(0, 1, 0)
    pack(1, 1, 0)
    pack(2, 1, 0)
    pack(0, 1, 1)
    pack(1, 1, 1)
    pack(2, 1, 1)
    send((1, 2, 0), (3, 2, 0))
    for j in range(3):
        pack(j, 0, 1)
    send((1, 2, 1), (3, 2, 1))
    fetch.wait()
    for j in range(3):
        pack(j, 0, 0)
        order_rows(j)
    send((2, 1, 0), (2, 1, 1), (2, 3, 0), (2, 3, 1))
    send((2, 2, 0), (2, 2, 1))

    got = set()

    def solve_ready(j, rc):
        for t, e in every:
            if t + e and (j, t, e) not in got:
                got.add((j, t, e))
                forward_copy(j, t, e).wait_recv()
        for rb in range(4):
            for ra in range(2):
                need(j, (rc, rb, ra))
        solve(j, rc)

    for j in range(3):
        solve_ready(j, 0)
    for j in range(3):
        solve_ready(j, 1)
    for rc in (3, 2):
        for j in range(3):
            solve_ready(j, rc)
    stores = []
    for j in range(3):
        for t, e in every:
            for rc in range(4):
                if t + e:
                    return_copy(j, t, e, rc).wait_recv()
            l = list_id(j, t, e)
            stores.append(pltpu.make_async_copy(YR.at[l], yr_out.at[l], out_sem.at[l]))
            stores[-1].start()
    for store in stores:
        store.wait()
    table_store.wait()
    for copy in sent:
        copy.wait_send()


def exchange(inverses, state, height, pressure, lows, held):
    any_space = pl.BlockSpec(memory_space=pl.ANY)
    smem = pl.BlockSpec(memory_space=pltpu.SMEM)
    messages = pltpu.VMEM((12, 4, MSG, 128), BF16)
    return pl.pallas_call(
        exchange_kernel,
        out_shape=(
            jax.ShapeDtypeStruct((12, 4, MSG, 128), BF16),
            jax.ShapeDtypeStruct((48, 128), jnp.int32),
        ),
        in_specs=[any_space] * 2 + [pl.BlockSpec(memory_space=pltpu.VMEM)] * 2 + [smem, smem],
        out_specs=(any_space, any_space),
        scratch_shapes=[
            pltpu.VMEM(inverses.shape, BF16),
            pltpu.VMEM(state.shape, BF16),
            pltpu.VMEM((144, 2 * LEV + 1), BF16),
            pltpu.VMEM((3, 4, 4, 2, UNIT, 128), BF16),
            pltpu.VMEM((4, 4, 2, 4, 1, 128), jnp.int32),
            pltpu.SMEM((4, 4, 2, 4, 1, 128), jnp.int32),
            pltpu.VMEM((48, 128), jnp.int32),
            pltpu.SMEM((48, 128), jnp.int32),
            pltpu.VMEM((ROWS, 128), F32),
            pltpu.VMEM((ROWS, 128), F32),
            messages,
            messages,
            messages,
            messages,
            pltpu.VMEM((4, CHUNK, 128), F32),
            pltpu.VMEM((4, CHUNK, 128), F32),
            pltpu.VMEM((3, 4 * PAIR_ROWS, 128), jnp.int32),
            pltpu.SemaphoreType.DMA((5,)),
            pltpu.SemaphoreType.DMA((3, 4, 4, 2)),
            pltpu.SemaphoreType.DMA((3, 4, 4, 2)),
            pltpu.SemaphoreType.DMA((13,)),
            pltpu.SemaphoreType.DMA((13,)),
            pltpu.SemaphoreType.DMA((12,)),
            pltpu.SemaphoreType.DMA((12,)),
            pltpu.SemaphoreType.DMA((12, 4)),
            pltpu.SemaphoreType.DMA((12, 4)),
            pltpu.SemaphoreType.DMA((12,)),
        ],
        compiler_params=pltpu.CompilerParams(
            collective_id=0, has_side_effects=True, vmem_limit_bytes=60 * 1024 * 1024
        ),
    )(inverses, state, height, pressure, lows, held)


def finish_kernel(yr, table, held, state, response, mass, out, OP, YM, YT, TM, TR):
    @pl.when(pl.program_id(0) == 0)
    def _():
        def body(l, carry):
            for rc in range(4):
                TM[rc] = yr[l, rc, 0:CHUNK, :].astype(F32)
                tails = yr[l, rc, CHUNK:MSG, :].astype(F32)[0:PAIR_ROWS]
                for u in range(8):
                    TR[rc, PAIR_ROWS * u : PAIR_ROWS * (u + 1), :] = pltpu.roll(tails, 128 - 16 * u, 1) if u else tails
            for rc in range(4):
                for u in range(8):
                    for to, of, put, row in copy_items(table, 4 * l + rc, u, (YM, YT), (TM.at[rc], TR.at[rc])):
                        to[pl.ds(row, 2), :] = of[put : put + 2, :]
            return carry

        lax.fori_loop(0, 12, body, 0)
        row = lax.broadcasted_iota(jnp.int32, OP.shape, 0)
        col = lax.broadcasted_iota(jnp.int32, OP.shape, 1)
        down = (
            lax.broadcasted_iota(jnp.int32, (OP.shape[0], LEV), 0)
            == lax.broadcasted_iota(jnp.int32, (OP.shape[0], LEV), 1) + LEV
        ).astype(BF16)
        across = (
            lax.broadcasted_iota(jnp.int32, (LEV, 256), 0) == lax.broadcasted_iota(jnp.int32, (LEV, 256), 1)
        ).astype(BF16)
        wide = jnp.dot(response[...], across, preferred_element_type=F32).astype(BF16)
        lower = jnp.dot(down, wide, preferred_element_type=F32)
        masses = jnp.dot(jnp.broadcast_to(mass[...][None, :], (16, LEV)), across, preferred_element_type=F32)[0:1]
        upper = jnp.where((row == col) & (col < LEV), 1.0, 0.0)
        OP[...] = jnp.where(row < LEV, upper, jnp.where(row == 2 * LEV, -masses, -lower)).astype(BF16)

    rows = pl.ds(pl.multiple_of(pl.program_id(0) * TILE, TILE), TILE)
    nt = (((1,), (1,)), ((), ()))
    lanes = lax.broadcasted_iota(jnp.int32, (TILE, 128), 1)
    tail = jnp.where(lanes < REM, YT[rows, :], 0.0).astype(BF16)
    columns = jnp.concatenate([YM[rows, :].astype(BF16), tail], axis=1)
    total = lax.dot_general(OP[...], columns, nt, preferred_element_type=F32)[0 : 2 * LEV + 1]
    level = lax.broadcasted_iota(jnp.int32, total.shape, 0)
    total += jnp.where(level < LEV, 0.0, state[...].astype(F32))
    col = pl.program_id(0) * TILE + lax.broadcasted_iota(jnp.int32, (1, TILE), 1)
    order = jnp.full((1, TILE), held[0], jnp.int32)
    for s in range(1, SLOTS):
        order = jnp.where(col >= s * WIDTH, held[s], order)
    out[...] = jnp.where(order >= 0, total, 0.0).astype(BF16)


def finish(yr, table, held, state, response, mass):
    smem = pl.BlockSpec(memory_space=pltpu.SMEM)
    rows = state.shape[0]
    block = pl.BlockSpec((rows, TILE), lambda i: (0, i))
    return pl.pallas_call(
        finish_kernel,
        grid=(TILES,),
        out_shape=jax.ShapeDtypeStruct(state.shape, BF16),
        in_specs=[
            pl.BlockSpec((12, 4, MSG, 128), lambda i: (0, 0, 0, 0)),
            smem,
            smem,
            block,
            pl.BlockSpec((LEV, LEV), lambda i: (0, 0)),
            pl.BlockSpec((LEV,), lambda i: (0,)),
        ],
        out_specs=block,
        scratch_shapes=[
            pltpu.VMEM((288, 256), BF16),
            pltpu.VMEM((TILE * TILES, 128), F32),
            pltpu.VMEM((TILE * TILES, 128), F32),
            pltpu.VMEM((4, CHUNK, 128), F32),
            pltpu.VMEM((4, CHUNK, 128), F32),
        ],
        compiler_params=pltpu.CompilerParams(vmem_limit_bytes=60 * 1024 * 1024),
    )(yr, table, held, state, response, mass)


def shards(
    state,
    held_orders,
    pair_lows,
    inverses,
    height_operator,
    pressure_column,
    thermal_response_matrix,
    mass_row,
):
    yr, table = exchange(jnp.swapaxes(inverses, 1, 2), state, height_operator, pressure_column, pair_lows, held_orders)
    return finish(yr, table, held_orders, state, thermal_response_matrix, mass_row)


def solution(mesh):
    torus = Mesh(mesh.devices.reshape(4, 4, 4, 2), AXES)
    columns = P(None, AXES)
    placed = (columns, P(AXES), P(AXES), P(AXES, None, None, None), P(), P(), P(), P())
    return jax.shard_map(shards, mesh=torus, in_specs=placed, out_specs=columns, check_vma=False)
```

```python
import functools

import jax
import jax.numpy as jnp
from jax import lax
from jax.experimental import pallas as pl
from jax.experimental.pallas import tpu as pltpu
from jax.sharding import Mesh
from jax.sharding import PartitionSpec as P

AXES = ("grp", "wave_0", "wave_1", "wave_2")
MESH = pl.DeviceIdType.MESH
BF16 = jnp.bfloat16
F32 = jnp.float32
LEV = 137
REM = LEV - 128
HALF = 384
TRUNC = 767
SLOTS = 5
WIDTH = 2 * (TRUNC + 2)
COLS = SLOTS * WIDTH
ROWS = 8192
MISS = ROWS - 8
PAIR_ROWS = 24
CHUNK = 8 * PAIR_ROWS
MSG = 224
UNIT = 320
STRIP = 2 * REM
PER_ROW = 7
BLOCK = 768
BLOCKS = 10
TAIL_COLS = COLS - BLOCK * BLOCKS
TILE = 2048
TILES = 4


def list_id(j, t, e):
    return j * 4 + t * 2 + e


def partner(core, p):
    even = p % 2
    return (1 - core) * (p + 1 - 2 * even) + core * (3 - p)


def solver_coords(pos, core, j, t, e):
    dest_core = (core + e) % 2
    pa = pos[j] if t == 0 else partner(dest_core, pos[j])
    return [pa if d == j else pos[d] for d in range(3)], dest_core


def source_coords(pos, core, j, rc, rb, ra):
    a, b, c = j, (j + 1) % 3, (j + 2) % 3
    out = [None, None, None]
    pa = pos[a]
    out[a] = pa + ra * (partner(1 - core, pa) - pa)
    out[b] = (pos[b] + 4 - rb) % 4
    out[c] = (pos[c] + 4 - rc) % 4
    return out


def copy_items(table, line, u, target, source):
    for t in range(2 * SLOTS + 1):
        put = PAIR_ROWS * u + 2 * t
        row = table[line, 16 * u + t]
        for to, of in zip(target, source):
            yield to, of, put, row


def exchange_kernel(
    inv_hbm, state_hbm, height, pressure, lows, held,
    yr_out, table_out,
    RAW, STATE, DRIVE, G, META, METAS, TABLE, TABLES, XM, XR, SND, RCV, YS, YR, TM, TR, MV,
    in_sem, g_send, g_recv, m_send, m_recv, f_send, f_recv, b_send, b_recv, out_sem,
):
    pos = [lax.axis_index(AXES[d]) for d in range(3)]
    core = lax.axis_index(AXES[3])

    def device(coords, c):
        return {AXES[0]: coords[0], AXES[1]: coords[1], AXES[2]: coords[2], AXES[3]: c}

    def shifted(d, delta):
        return [(pos[k] + 4 + delta) % 4 if k == d else pos[k] for k in range(3)]

    loads = [
        pltpu.make_async_copy(inv_hbm, RAW, in_sem.at[0]),
        pltpu.make_async_copy(state_hbm, STATE, in_sem.at[1]),
    ]
    for load in loads:
        load.start()

    barrier = pltpu.get_barrier_semaphore()
    other = 1 - core
    peers = [(pos, other)]
    for d in range(3):
        for delta in (1, -1):
            peers.append((shifted(d, delta), core))
            peers.append((shifted(d, delta), other))
        peers.append((shifted(d, 2), core))
    peers.append((shifted(0, 2), other))

    for coords, c in peers:
        pl.semaphore_signal(barrier, inc=1, device_id=device(coords, c), device_id_type=MESH)

    lane1 = lax.broadcasted_iota(jnp.int32, (1, 128), 1)
    record = jnp.zeros((1, 128), jnp.int32)
    for k in range(3):
        record = jnp.where(lane1 == k, lows[k], record)
    for k in range(SLOTS):
        record = jnp.where(lane1 == 8 + k, held[k], record)
    META[pos[2], pos[1], core, pos[0]] = record

    def chosen(rows, cols, test):
        r = lax.broadcasted_iota(jnp.int32, (rows, cols), 0)
        c = lax.broadcasted_iota(jnp.int32, (rows, cols), 1)
        return test(r, c).astype(BF16)

    below = chosen(16, LEV, lambda r, c: c == r + 128)
    beside = chosen(LEV, 128, lambda r, c: r == c + 128)
    loads[0].wait()
    for j in range(3):
        strips = [jnp.zeros((16, 128), F32)] * 2
        for h in range(2):
            raw = RAW[j, :, h, :]
            bottom = jnp.dot(below, raw, preferred_element_type=F32).astype(BF16)
            right = jnp.dot(raw, beside, preferred_element_type=F32)
            corner = jnp.dot(bottom, beside, preferred_element_type=F32)
            G[j, 0, 0, 0, 128 * h : 128 * (h + 1), :] = raw[0:128, 0:128]
            G[j, 0, 0, 0, 256 + 16 * h : 272 + 16 * h, :] = bottom[:, 0:128]
            for g in range(9):
                part = right[16 * g : 16 * (g + 1)] if g < 8 else corner
                shift = STRIP * (g % PER_ROW) + REM * h
                strips[g // PER_ROW] += pltpu.roll(part, shift, 1) if shift else part
        for k in range(2):
            G[j, 0, 0, 0, 288 + 16 * k : 304 + 16 * k, :] = strips[k].astype(BF16)
    pl.semaphore_wait(barrier, len(peers))

    def unit_copy(j, dest):
        rc, rb, ra = dest
        a, b, c = j, (j + 1) % 3, (j + 2) % 3
        if dest == (0, 0, 1):
            src = (0, 0, 0)
            coords = [partner(1 - core, pos[k]) if k == a else pos[k] for k in range(3)]
        elif rc == 0:
            ring, step, k = b, rb, 1
        else:
            ring, step, k = c, rc, 0
        if dest != (0, 0, 1):
            forward = {1: (0, 1), 3: (0, -1), 2: (1, 1) if ra == 0 else (3, -1)}[step]
            src = list(dest)
            src[k] = forward[0]
            src = tuple(src)
            coords = shifted(ring, forward[1])
        return src, pltpu.make_async_remote_copy(
            src_ref=G.at[(j,) + src],
            dst_ref=G.at[(j,) + dest],
            send_sem=g_send.at[(j,) + dest],
            recv_sem=g_recv.at[(j,) + dest],
            device_id=device(coords, core),
            device_id_type=MESH,
        )

    here = {(j, 0, 0, 0) for j in range(3)}
    sent = []

    def need(j, unit):
        if (j,) + unit not in here:
            here.add((j,) + unit)
            unit_copy(j, unit)[1].wait_recv()

    def send(*dests):
        for dest in dests:
            for j in range(3):
                src, copy = unit_copy(j, dest)
                need(j, src)
                copy.start()
                sent.append(copy)

    def meta_copies(stage):
        if stage == 0:
            index = (pos[2], pos[1], core, pos[0])
            out = [(index, device(shifted(0, delta), core), delta - 1) for delta in (1, 2, 3)]
            return out + [(index, device(shifted(0, delta), other), 3 + delta) for delta in range(4)]
        index = (pos[2], pos[1])[: 3 - stage]
        return [(index, device(shifted(stage, delta), core), 3 + 3 * stage + delta) for delta in (1, 2, 3)]

    def meta_copy(index, dev, sem):
        ref = META.at[index]
        return pltpu.make_async_remote_copy(
            src_ref=ref, dst_ref=ref, send_sem=m_send.at[sem], recv_sem=m_recv.at[sem],
            device_id=dev, device_id_type=MESH,
        )

    def meta_start(stage):
        for item in meta_copies(stage):
            copy = meta_copy(*item)
            copy.start()
            sent.append(copy)

    def meta_wait(stage):
        for item in meta_copies(stage):
            meta_copy(*item).wait_recv()

    orders = [held[s] for s in range(SLOTS)]
    eye = (
        lax.broadcasted_iota(jnp.int32, (128, 128), 0) == lax.broadcasted_iota(jnp.int32, (128, 128), 1)
    ).astype(BF16)
    nt = (((1,), (1,)), ((), ()))

    def turn(all_rows, base, width):
        drive = jnp.dot(DRIVE[0:144, :], all_rows, preferred_element_type=F32)
        col = base + lax.broadcasted_iota(jnp.int32, (1, width), 1)
        order = jnp.full((1, width), orders[0], jnp.int32)
        start = jnp.zeros((1, width), jnp.int32)
        for s in range(1, SLOTS):
            order = jnp.where(col >= s * WIDTH, orders[s], order)
            start = jnp.where(col >= s * WIDTH, s * WIDTH, start)
        q = (col - start) // 2
        degree = jnp.where(q <= TRUNC - order, order + q, q - 1)
        scale = (degree * (degree + 1)).astype(F32) / float(TRUNC * (TRUNC + 1))
        level = lax.broadcasted_iota(jnp.int32, (144, width), 0)
        divergence = jnp.where(level < LEV, all_rows[0:144].astype(F32), 0.0)
        right = (divergence + scale * drive).astype(BF16)
        for k in range(width // 128):
            out = lax.dot_general(eye, right[:, 128 * k : 128 * (k + 1)], nt, preferred_element_type=F32)
            rows = pl.ds(pl.multiple_of(base + 128 * k, 128), 128)
            XM[rows, :] = out[:, 0:128]
            XR[rows, 0:16] = out[:, 128:144]

    def turn_blocks(first, last):
        def body(i, carry):
            base = pl.multiple_of(i * BLOCK, BLOCK)
            turn(STATE[:, pl.ds(base, BLOCK)], base, BLOCK)
            return carry

        lax.fori_loop(first, last, body, 0)

    meta_start(0)
    send((0, 0, 1), (0, 1, 0), (0, 3, 0), (1, 0, 0), (3, 0, 0))
    TM[...] = jnp.zeros_like(TM)
    TR[...] = jnp.zeros_like(TR)
    XM[MISS - 504 : ROWS, :] = jnp.zeros((512, 128), F32)
    XR[...] = jnp.zeros_like(XR)
    rows = 2 * LEV + 1
    diagonal = chosen(LEV, LEV, lambda r, c: r == c) * jnp.broadcast_to(pressure[...][None, :], (LEV, LEV))
    thermal_rows = chosen(LEV, rows, lambda r, c: c == r + LEV)
    pressure_row = chosen(LEV, rows, lambda r, c: c == 2 * LEV)
    DRIVE[...] = jnp.zeros_like(DRIVE)
    DRIVE[0:LEV, :] = (
        jnp.dot(height[...], thermal_rows, preferred_element_type=F32)
        + jnp.dot(diagonal, pressure_row, preferred_element_type=F32)
    ).astype(BF16)
    loads[1].wait()
    turn_blocks(0, 7)
    meta_wait(0)
    meta_start(1)
    send((0, 1, 1), (0, 3, 1), (1, 0, 1), (3, 0, 1))
    turn_blocks(7, 10)
    last = jnp.concatenate([STATE[:, BLOCK * BLOCKS : COLS], jnp.zeros((rows, 128 - TAIL_COLS), BF16)], axis=1)
    turn(last, BLOCK * BLOCKS, 128)
    meta_wait(1)
    meta_start(2)
    send((0, 2, 0), (1, 1, 0), (3, 1, 0), (1, 3, 0), (3, 3, 0))
    send((0, 2, 1), (1, 1, 1), (3, 1, 1), (1, 3, 1), (3, 3, 1))
    meta_wait(2)
    fetch = pltpu.make_async_copy(META, METAS, in_sem.at[2])
    fetch.start()

    def low_of(coords, c, j):
        return METAS[coords[2], coords[1], c, coords[0], 0, j]

    every = [(t, e) for t in (1, 0) for e in (0, 1)]

    for j in range(3):
        for t, e in every:
            dest, dest_core = solver_coords(pos, core, j, t, e)
            for rc in range(4):
                line = jnp.zeros((1, 128), jnp.int32)
                for u in range(8):
                    src = source_coords(dest, dest_core, j, rc, u // 2, u % 2)
                    entry = META[src[2], src[1], dest_core, src[0]]
                    line = jnp.where(lane1 // 16 == u, jnp.broadcast_to(entry[:, j : j + 1], (1, 128)), line)
                at = 4 * list_id(j, t, e) + rc
                TABLE[at : at + 1, :] = line
    low = TABLE[...]
    item = lax.broadcasted_iota(jnp.int32, (48, 128), 1) % 16
    order = jnp.zeros((48, 128), jnp.int32)
    extra = jnp.full((48, 128), MISS, jnp.int32)
    for s in range(SLOTS):
        order = jnp.where((item == s) | (item == SLOTS + s), orders[s], order)
        extra = jnp.where(low == orders[s], s * WIDTH + 2 * (TRUNC + 1 - low), extra)
    first = jnp.where(order <= low, 2 * (low - order), 2 * (TRUNC + 1 - low)) + item * WIDTH
    second = 2 * (TRUNC - low - order) + (item - SLOTS) * WIDTH
    TABLE[...] = jnp.where(item < SLOTS, first, jnp.where(item < 2 * SLOTS, second, extra))
    table = pltpu.make_async_copy(TABLE, TABLES, in_sem.at[3])
    table.start()
    table_store = pltpu.make_async_copy(TABLE, table_out, in_sem.at[4])
    table_store.start()
    send((2, 0, 0), (2, 0, 1))
    table.wait()

    def pack(j, t, e):
        dest, dest_core = solver_coords(pos, core, j, t, e)
        l = list_id(j, t, e)
        target = RCV if t + e == 0 else SND

        for rc in range(4):
            for u in range(8):
                for to, of, put, row in copy_items(TABLES, 4 * l + rc, u, (TM.at[rc], TR.at[rc]), (XM, XR)):
                    to[put : put + 2, :] = of[pl.ds(row, 2), :]
            target[l, rc, 0:CHUNK, :] = TM[rc].astype(BF16)
            tail = TR[rc, 0:PAIR_ROWS, :]
            for u in range(1, 8):
                tail += pltpu.roll(TR[rc, PAIR_ROWS * u : PAIR_ROWS * (u + 1), :], 16 * u, 1)
            tail = jnp.concatenate([tail, jnp.zeros((MSG - CHUNK - PAIR_ROWS, 128), F32)], axis=0)
            target[l, rc, CHUNK:MSG, :] = tail.astype(BF16)

        if t + e:
            copy = forward_copy(j, t, e)
            copy.start()
            sent.append(copy)

    def forward_copy(j, t, e):
        dest, dest_core = solver_coords(pos, core, j, t, e)
        l = list_id(j, t, e)
        return pltpu.make_async_remote_copy(
            src_ref=SND.at[l], dst_ref=RCV.at[l], send_sem=f_send.at[l], recv_sem=f_recv.at[l],
            device_id=device(dest, dest_core), device_id_type=MESH,
        )

    def origin(j, t, e):
        pa = pos[j] if t == 0 else partner(core, pos[j])
        return [pa if d == j else pos[d] for d in range(3)], (core + e) % 2

    def return_copy(j, t, e, rc):
        l = list_id(j, t, e)
        coords, c = origin(j, t, e)
        return pltpu.make_async_remote_copy(
            src_ref=YS.at[l, rc], dst_ref=YR.at[l, rc], send_sem=b_send.at[l, rc], recv_sem=b_recv.at[l, rc],
            device_id=device(coords, c), device_id_type=MESH,
        )

    row_id = lax.broadcasted_iota(jnp.int32, (PAIR_ROWS, 128), 0)

    def order_rows(j):
        for t, e in every:
            coords, c = origin(j, t, e)
            rows = jnp.full((PAIR_ROWS, 128), HALF + 1, jnp.int32)
            for s in range(SLOTS):
                order = METAS[coords[2], coords[1], c, coords[0], 0, 8 + s]
                rows = jnp.where(row_id // 2 == s, order, rows)
            MV[j, PAIR_ROWS * (2 * t + e) : PAIR_ROWS * (2 * t + e + 1), :] = rows

    lane = lax.broadcasted_iota(jnp.int32, (4 * PAIR_ROWS, 128), 1)

    def solve(j, rc):
        tails = jnp.concatenate(
            [RCV[list_id(j, k // 2, k % 2), rc, CHUNK:MSG, :].astype(F32)[:PAIR_ROWS] for k in range(4)], axis=0
        )
        spread = jnp.zeros((4 * PAIR_ROWS, 128), F32)
        for rb in range(4):
            rows = slice(2 * PAIR_ROWS * rb, 2 * PAIR_ROWS * (rb + 1))
            mains = [RCV[list_id(j, k // 2, k % 2), rc, rows, :].astype(F32) for k in range(4)]
            solved = []
            for ra in range(2):
                u = 2 * rb + ra
                low = low_of(source_coords(pos, core, j, rc, rb, ra), core, j)
                unit = G.at[j, rc, rb, ra]
                x = jnp.concatenate([m[PAIR_ROWS * ra : PAIR_ROWS * (ra + 1)] for m in mains], axis=0)
                is_low = MV[j] <= low
                main = jnp.concatenate([jnp.where(is_low, x, 0.0), jnp.where(is_low, 0.0, x)], axis=1).astype(BF16)
                tail_low = pltpu.roll(tails, 128 - 16 * u, 1) if u else tails
                tail_high = pltpu.roll(tails, (128 + REM - 16 * u) % 128, 1)
                tail = jnp.where(
                    lane < REM,
                    jnp.where(is_low, tail_low, 0.0),
                    jnp.where(lane < STRIP, jnp.where(is_low, 0.0, tail_high), 0.0),
                ).astype(BF16)
                strips = [unit[288:304, :].astype(F32), unit[304:320, :].astype(F32)]
                strip = jnp.concatenate(
                    [
                        pltpu.roll(strips[g // PER_ROW], 128 - STRIP * (g % PER_ROW), 1)
                        if g % PER_ROW
                        else strips[g // PER_ROW]
                        for g in range(9)
                    ],
                    axis=0,
                ).astype(BF16)
                weights = jnp.concatenate(
                    [
                        jnp.concatenate([unit[0:128, :], unit[128:256, :]], axis=1),
                        jnp.concatenate([unit[256:272, :], unit[272:288, :]], axis=1),
                    ],
                    axis=0,
                )
                y = lax.dot_general(main, weights, nt, preferred_element_type=F32) + lax.dot_general(
                    tail, strip, nt, preferred_element_type=F32
                )
                solved.append(y[:, 0:128])
                wide = jnp.concatenate([y[:, 128:144], jnp.zeros((4 * PAIR_ROWS, 112), F32)], axis=1)
                shifted_tail = pltpu.roll(wide, 16 * u, 1) if u else wide
                keep = (lane >= 16 * u) & (lane < 16 * u + REM)
                spread += jnp.where(keep, shifted_tail, 0.0)
            for k in range(4):
                l = list_id(j, k // 2, k % 2)
                part = slice(PAIR_ROWS * k, PAIR_ROWS * (k + 1))
                (YR if k == 0 else YS)[l, rc, rows, :] = jnp.concatenate(
                    [solved[0][part], solved[1][part]], axis=0
                ).astype(BF16)
        for k in range(4):
            l = list_id(j, k // 2, k % 2)
            part = jnp.concatenate(
                [spread[PAIR_ROWS * k : PAIR_ROWS * (k + 1), :], jnp.zeros((MSG - CHUNK - PAIR_ROWS, 128), F32)], axis=0
            )
            (YR if k == 0 else YS)[l, rc, CHUNK:MSG, :] = part.astype(BF16)
            if k:
                copy = return_copy(j, k // 2, k % 2, rc)
                copy.start()
                sent.append(copy)

    pack(0, 1, 0)
    pack(1, 1, 0)
    pack(2, 1, 0)
    pack(0, 1, 1)
    pack(1, 1, 1)
    pack(2, 1, 1)
    send((1, 2, 0), (3, 2, 0))
    for j in range(3):
        pack(j, 0, 1)
    send((1, 2, 1), (3, 2, 1))
    fetch.wait()
    for j in range(3):
        pack(j, 0, 0)
        order_rows(j)
    send((2, 1, 0), (2, 1, 1), (2, 3, 0), (2, 3, 1))
    send((2, 2, 0), (2, 2, 1))

    got = set()

    def solve_ready(j, rc):
        for t, e in every:
            if t + e and (j, t, e) not in got:
                got.add((j, t, e))
                forward_copy(j, t, e).wait_recv()
        for rb in range(4):
            for ra in range(2):
                need(j, (rc, rb, ra))
        solve(j, rc)

    for j in range(3):
        solve_ready(j, 0)
    for j in range(3):
        solve_ready(j, 1)
    for rc in (3, 2):
        for j in range(3):
            solve_ready(j, rc)
    stores = []
    for j in range(3):
        for t, e in every:
            for rc in range(4):
                if t + e:
                    return_copy(j, t, e, rc).wait_recv()
            l = list_id(j, t, e)
            stores.append(pltpu.make_async_copy(YR.at[l], yr_out.at[l], out_sem.at[l]))
            stores[-1].start()
    for store in stores:
        store.wait()
    table_store.wait()
    for copy in sent:
        copy.wait_send()


def exchange(inverses, state, height, pressure, lows, held):
    any_space = pl.BlockSpec(memory_space=pl.ANY)
    smem = pl.BlockSpec(memory_space=pltpu.SMEM)
    messages = pltpu.VMEM((12, 4, MSG, 128), BF16)
    return pl.pallas_call(
        exchange_kernel,
        out_shape=(
            jax.ShapeDtypeStruct((12, 4, MSG, 128), BF16),
            jax.ShapeDtypeStruct((48, 128), jnp.int32),
        ),
        in_specs=[any_space] * 2 + [pl.BlockSpec(memory_space=pltpu.VMEM)] * 2 + [smem, smem],
        out_specs=(any_space, any_space),
        scratch_shapes=[
            pltpu.VMEM(inverses.shape, BF16),
            pltpu.VMEM(state.shape, BF16),
            pltpu.VMEM((144, 2 * LEV + 1), BF16),
            pltpu.VMEM((3, 4, 4, 2, UNIT, 128), BF16),
            pltpu.VMEM((4, 4, 2, 4, 1, 128), jnp.int32),
            pltpu.SMEM((4, 4, 2, 4, 1, 128), jnp.int32),
            pltpu.VMEM((48, 128), jnp.int32),
            pltpu.SMEM((48, 128), jnp.int32),
            pltpu.VMEM((ROWS, 128), F32),
            pltpu.VMEM((ROWS, 128), F32),
            messages,
            messages,
            messages,
            messages,
            pltpu.VMEM((4, CHUNK, 128), F32),
            pltpu.VMEM((4, CHUNK, 128), F32),
            pltpu.VMEM((3, 4 * PAIR_ROWS, 128), jnp.int32),
            pltpu.SemaphoreType.DMA((5,)),
            pltpu.SemaphoreType.DMA((3, 4, 4, 2)),
            pltpu.SemaphoreType.DMA((3, 4, 4, 2)),
            pltpu.SemaphoreType.DMA((13,)),
            pltpu.SemaphoreType.DMA((13,)),
            pltpu.SemaphoreType.DMA((12,)),
            pltpu.SemaphoreType.DMA((12,)),
            pltpu.SemaphoreType.DMA((12, 4)),
            pltpu.SemaphoreType.DMA((12, 4)),
            pltpu.SemaphoreType.DMA((12,)),
        ],
        compiler_params=pltpu.CompilerParams(
            collective_id=0, has_side_effects=True, vmem_limit_bytes=60 * 1024 * 1024
        ),
    )(inverses, state, height, pressure, lows, held)


def finish_kernel(yr, table, held, state, response, mass, out, OP, YM, YT, TM, TR):
    @pl.when(pl.program_id(0) == 0)
    def _():
        def body(l, carry):
            for rc in range(4):
                TM[rc] = yr[l, rc, 0:CHUNK, :].astype(F32)
                tails = yr[l, rc, CHUNK:MSG, :].astype(F32)[0:PAIR_ROWS]
                for u in range(8):
                    TR[rc, PAIR_ROWS * u : PAIR_ROWS * (u + 1), :] = pltpu.roll(tails, 128 - 16 * u, 1) if u else tails
            for rc in range(4):
                for u in range(8):
                    for to, of, put, row in copy_items(table, 4 * l + rc, u, (YM, YT), (TM.at[rc], TR.at[rc])):
                        to[pl.ds(row, 2), :] = of[put : put + 2, :]
            return carry

        lax.fori_loop(0, 12, body, 0)
        row = lax.broadcasted_iota(jnp.int32, OP.shape, 0)
        col = lax.broadcasted_iota(jnp.int32, OP.shape, 1)
        down = (
            lax.broadcasted_iota(jnp.int32, (OP.shape[0], LEV), 0)
            == lax.broadcasted_iota(jnp.int32, (OP.shape[0], LEV), 1) + LEV
        ).astype(BF16)
        across = (
            lax.broadcasted_iota(jnp.int32, (LEV, 256), 0) == lax.broadcasted_iota(jnp.int32, (LEV, 256), 1)
        ).astype(BF16)
        wide = jnp.dot(response[...], across, preferred_element_type=F32).astype(BF16)
        lower = jnp.dot(down, wide, preferred_element_type=F32)
        masses = jnp.dot(jnp.broadcast_to(mass[...][None, :], (16, LEV)), across, preferred_element_type=F32)[0:1]
        upper = jnp.where((row == col) & (col < LEV), 1.0, 0.0)
        OP[...] = jnp.where(row < LEV, upper, jnp.where(row == 2 * LEV, -masses, -lower)).astype(BF16)

    rows = pl.ds(pl.multiple_of(pl.program_id(0) * TILE, TILE), TILE)
    nt = (((1,), (1,)), ((), ()))
    lanes = lax.broadcasted_iota(jnp.int32, (TILE, 128), 1)
    tail = jnp.where(lanes < REM, YT[rows, :], 0.0).astype(BF16)
    columns = jnp.concatenate([YM[rows, :].astype(BF16), tail], axis=1)
    total = lax.dot_general(OP[...], columns, nt, preferred_element_type=F32)[0 : 2 * LEV + 1]
    level = lax.broadcasted_iota(jnp.int32, total.shape, 0)
    total += jnp.where(level < LEV, 0.0, state[...].astype(F32))
    col = pl.program_id(0) * TILE + lax.broadcasted_iota(jnp.int32, (1, TILE), 1)
    order = jnp.full((1, TILE), held[0], jnp.int32)
    for s in range(1, SLOTS):
        order = jnp.where(col >= s * WIDTH, held[s], order)
    out[...] = jnp.where(order >= 0, total, 0.0).astype(BF16)


def finish(yr, table, held, state, response, mass):
    smem = pl.BlockSpec(memory_space=pltpu.SMEM)
    rows = state.shape[0]
    block = pl.BlockSpec((rows, TILE), lambda i: (0, i))
    return pl.pallas_call(
        finish_kernel,
        grid=(TILES,),
        out_shape=jax.ShapeDtypeStruct(state.shape, BF16),
        in_specs=[
            pl.BlockSpec((12, 4, MSG, 128), lambda i: (0, 0, 0, 0)),
            smem,
            smem,
            block,
            pl.BlockSpec((LEV, LEV), lambda i: (0, 0)),
            pl.BlockSpec((LEV,), lambda i: (0,)),
        ],
        out_specs=block,
        scratch_shapes=[
            pltpu.VMEM((288, 256), BF16),
            pltpu.VMEM((TILE * TILES, 128), F32),
            pltpu.VMEM((TILE * TILES, 128), F32),
            pltpu.VMEM((4, CHUNK, 128), F32),
            pltpu.VMEM((4, CHUNK, 128), F32),
        ],
        compiler_params=pltpu.CompilerParams(vmem_limit_bytes=60 * 1024 * 1024),
    )(yr, table, held, state, response, mass)


def shards(
    state,
    held_orders,
    pair_lows,
    inverses,
    height_operator,
    pressure_column,
    thermal_response_matrix,
    mass_row,
):
    yr, table = exchange(jnp.swapaxes(inverses, 1, 2), state, height_operator, pressure_column, pair_lows, held_orders)
    return finish(yr, table, held_orders, state, thermal_response_matrix, mass_row)


def solution(mesh):
    torus = Mesh(mesh.devices.reshape(4, 4, 4, 2), AXES)
    columns = P(None, AXES)
    placed = (columns, P(AXES), P(AXES), P(AXES, None, None, None), P(), P(), P(), P())
    return jax.shard_map(shards, mesh=torus, in_specs=placed, out_specs=columns, check_vma=False)
```
